256 devices in a mesh: seq: 16 (over z, core), head: 16 (over x, y).
Axes of the slice: x: 4, y: 4, z: 8, core: 2. Of those that a mesh axis runs over, the one named last changes fastest.
Arguments:
- tokens: bfloat16 [2048, 4096], P('seq', 'head'), may hold values from -6 to 6
- w_query: bfloat16 [4096, 4096], P(None, 'head'), may hold values from -0.09375 to 0.09375
- w_key: bfloat16 [4096, 4096], P(None, 'head'), may hold values from -0.09375 to 0.09375
- w_value: bfloat16 [4096, 4096], P(None, 'head'), may hold values from -0.09375 to 0.09375
- upstream: bfloat16 [2048, 4096], P('seq', 'head'), may hold values from -6 to 6
- log_decay: float32 [2048, 32], P('seq', 'head'), may hold values from -1 to 0, as said below
- segment: int32 [2048], replicated, may hold values from 0 to 7, never falling along the last dimension, each value on 1 to 512 neighbouring positions
Outputs:
- grad_query: bfloat16 [4096, 4096], P('seq', 'head')
- grad_key: bfloat16 [4096, 4096], P('seq', 'head')
- grad_value: bfloat16 [4096, 4096], P('seq', 'head')
The draws below stay inside these ranges and needn't reach their ends.
Inputs may be any that keep to these rules, and one draw needn't show every extreme that they name: log_decay is negative. `segment`: document ids never fall along the tokens; each document holds 1 to 512 tokens.
All inputs are finite; a program needn't handle non-finite values.
Results may differ from the reference program's by a relative error of at most 0.02.
Values may be sent and summed in bfloat16 or wider, within the bound.
A program may use at most 64 MiB of HBM per device.

```python
import math
import jax
import jax.numpy as jnp
import numpy as np
from jax import lax

D = 4096
HEAD_COUNT = 32
HEAD = 128
TOK_DEV = 128
DOCS = 8
TOKEN_COUNT = 2048
N_SEQ = 16


def draw_log_decay(key, part):
    document_lanes = jax.random.split(key, 6)
    fast_share = 0.5
    fast = jax.random.uniform(document_lanes[0], (HEAD_COUNT,)) < fast_share
    slow_rate = jax.random.uniform(document_lanes[1], (HEAD_COUNT,), minval=0.1, maxval=0.4) * math.log(10.0) / TOKEN_COUNT
    fast_rate = 1.0 / jax.random.uniform(document_lanes[2], (HEAD_COUNT,), minval=30.0, maxval=50.0)
    decay_rate = jnp.where(fast, fast_rate, slow_rate)
    coarse_estimate = jnp.exp(jax.random.uniform(document_lanes[3], (TOKEN_COUNT, HEAD_COUNT), minval=-math.log(2.0), maxval=math.log(2.0)))
    decay_jump = jax.random.uniform(document_lanes[4], (TOKEN_COUNT, HEAD_COUNT)) < 2.0 / TOKEN_COUNT
    feature_depth = jax.random.uniform(document_lanes[5], (TOKEN_COUNT, HEAD_COUNT), minval=0.22, maxval=0.69)
    return (-(decay_rate[None, :] * coarse_estimate) - jnp.where(decay_jump, feature_depth, 0.0)).astype(jnp.float32)


def strengthened(values, stream_key, source, target, parts, factor):
    owner, partner = [(jnp.arange(values.shape[dim]) // (values.shape[dim] // parts)).reshape([-1 if axis == dim else 1 for axis in range(values.ndim)]) for dim in (source, target)]
    chosen = jax.random.permutation(stream_key, parts)[partner]
    strong = (owner == chosen) | (owner == (partner + parts // 2) % parts)
    return jnp.where(strong, factor * values, values)


def steps_of(key, extent, cuts, smallest, high):
    def one(axis_at, blocks):
        draws = jax.random.uniform(jax.random.fold_in(jax.random.fold_in(key, 6), axis_at), (blocks,), jnp.float32, smallest / len(cuts), high / len(cuts))
        return jnp.repeat(jnp.exp(draws), extent[axis_at] // blocks).reshape((-1,) + (1,) * (len(extent) - axis_at - 1))

    gain = one(*cuts[0])
    for cut in cuts[1:]:
        gain = gain * one(*cut)
    return gain


def profile(count, total, limit, lean):
    weights = [(1 << 20) // math.isqrt(rank ** lean) + 1 for rank in range(2, count + 1)]
    surplus, holding = total - limit - (count - 1), [1] * (count - 1)
    while surplus > 0:
        movable = [i for i in range(count - 1) if holding[i] < limit]
        pool, remaining = sum([weights[i] for i in movable]), surplus
        for i in movable:
            more = min(limit - holding[i], max(1, remaining * weights[i] // pool), surplus)
            holding[i] = holding[i] + more
            surplus = surplus - more
    return np.array([limit] + holding)


def uneven(rng, number_of, total, reach, lean):
    if number_of == 2:
        one = jax.random.randint(rng, (), max(1, total - reach), min(reach, total - 1) + 1)
        return jnp.stack([one, total - one])
    tallies = jnp.asarray(profile(number_of, total, reach, lean), jnp.int32)
    pairs = (number_of - 1) // 2
    donor, taker = tallies[1:1 + 2 * pairs:2], tallies[2:2 + 2 * pairs:2]
    room = jnp.minimum(donor - 1, reach - taker)
    moved = jax.random.randint(jax.random.fold_in(rng, 1), (pairs,), 0, 1 << 20) % (room + 1)
    tallies = tallies.at[1:1 + 2 * pairs:2].set(donor - moved).at[2:2 + 2 * pairs:2].set(taker + moved)
    return tallies[jax.random.permutation(jax.random.fold_in(rng, 2), number_of)]


def scatter_about(own_key, dims, scale, reach, cuts=(), kind=jnp.bfloat16):
    result = scale * jax.random.normal(own_key, dims, jnp.float32)
    if cuts:
        result = result * steps_of(own_key, dims, cuts, -0.22, 0.18)
    return jnp.clip(result, -reach, reach).astype(kind)


def heavy_noise(rng, extent, scale, reach, shards, heavy, held_as=jnp.bfloat16):
    values = scale * jax.random.normal(rng, extent, jnp.float32)
    if shards:
        values = values * steps_of(rng, extent, shards, -0.22, 0.18)
    return jnp.clip(strengthened(values, jax.random.fold_in(rng, 3), *heavy), -reach, reach).astype(held_as)


def setup_inputs(seed: int = 0) -> dict:
    key_list = jax.random.split(jax.random.key(seed), 8)
    return {
        "tokens": heavy_noise(key_list[0], (TOKEN_COUNT, D), 1.0, 6.0, ((0, 16), (1, 16)), (0, 1, 16, 2.0)),
        "w_query": scatter_about(key_list[1], (D, HEAD_COUNT * HEAD), D ** -0.5, 0.09375, ((1, 16),)),
        "w_key": scatter_about(key_list[2], (D, HEAD_COUNT * HEAD), D ** -0.5, 0.09375, ((1, 16),)),
        "w_value": scatter_about(key_list[3], (D, HEAD_COUNT * HEAD), D ** -0.5, 0.09375, ((1, 16),)),
        "upstream": scatter_about(key_list[4], (TOKEN_COUNT, HEAD_COUNT * HEAD), 1.0, 6.0, ((0, 16), (1, 16))),
        "log_decay": draw_log_decay(jax.random.fold_in(key_list[7], 71), 0),
        "segment": jnp.searchsorted(jnp.cumsum(uneven(key_list[6], DOCS, TOKEN_COUNT, TOKEN_COUNT // 4, 0)), jnp.arange(TOKEN_COUNT), side="right").astype(jnp.int32),
    }


def rounded(array):
    return lax.optimization_barrier(array.astype(jnp.bfloat16)).astype(jnp.float32)

def block_factors(log_rates, segs, previous):
    log_sum = jnp.cumsum(log_rates, axis=0)
    last_sum = log_sum[-1]
    last_seg = segs[-1]
    state_entering = jnp.where((segs == previous)[:, None], jnp.exp(log_sum), 0.0)
    state_leaving = jnp.where((segs == last_seg)[:, None], jnp.exp(last_sum[None, :] - log_sum), 0.0)
    carry_decay = jnp.where(last_seg == previous, jnp.exp(last_sum), 0.0)
    places = jnp.arange(segs.shape[0], dtype=jnp.int32)
    same = (segs[:, None] == segs[None, :]) & (places[:, None] >= places[None, :])
    spread = log_sum.T[:, :, None] - log_sum.T[:, None, :]
    decay_mat = jnp.where(same[None], HEAD ** (-0.5) * jnp.exp(jnp.where(same[None], spread, 0.0)), 0.0)
    return (state_entering, state_leaving, carry_decay, decay_mat)

def summaries(block):
    query, key_rows, value_rows, upstream, log_rates, segs, previous = block
    state_entering, state_leaving, carry_decay, decay_mat = block_factors(log_rates, segs, previous)
    scale = HEAD ** (-0.5)
    weighted_keys = rounded(scale * state_leaving[:, :, None] * key_rows.astype(jnp.float32))
    segment_state = jnp.einsum('bdw,bdq->dwq', weighted_keys, value_rows.astype(jnp.float32), precision=lax.Precision.HIGHEST)
    weighted_queries = rounded(scale * state_entering[:, :, None] * query.astype(jnp.float32))
    following_state = jnp.einsum('bdw,bdq->dwq', weighted_queries, upstream.astype(jnp.float32), precision=lax.Precision.HIGHEST)
    return (carry_decay, segment_state, following_state)

def block_grads(block):
    query, key_rows, value_rows, upstream, log_rates, segs, previous, arriving_state, backward_state = block
    state_entering, state_leaving, carry_decay, decay_mat = block_factors(log_rates, segs, previous)
    query_rows_float = query.astype(jnp.float32)
    key_rows_float = key_rows.astype(jnp.float32)
    value_rows_float = value_rows.astype(jnp.float32)
    upstream_float = upstream.astype(jnp.float32)
    upper_limit = lax.Precision.HIGHEST
    attention_query_key = rounded(decay_mat * jnp.einsum('thd,shd->hts', query_rows_float, key_rows_float, precision=upper_limit))
    attention_upstream = rounded(decay_mat * jnp.einsum('thd,shd->hts', upstream_float, value_rows_float, precision=upper_limit))
    query_gradient = jnp.einsum('wcz,zwm->cwm', attention_upstream, key_rows_float, precision=upper_limit) + state_entering[:, :, None] * jnp.einsum('pzo,zao->pza', upstream_float, arriving_state, precision=upper_limit)
    key_gradient = jnp.einsum('voi,ovw->ivw', attention_upstream, query_rows_float, precision=upper_limit) + state_leaving[:, :, None] * jnp.einsum('ixz,xqz->ixq', value_rows_float, backward_state, precision=upper_limit)
    value_gradient = jnp.einsum('voi,ovw->ivw', attention_query_key, upstream_float, precision=upper_limit) + state_leaving[:, :, None] * jnp.einsum('dqg,qgf->dqf', key_rows_float, backward_state, precision=upper_limit)
    return (query_gradient.astype(jnp.bfloat16), key_gradient.astype(jnp.bfloat16), value_gradient.astype(jnp.bfloat16))

def reference(tokens, w_query, w_key, w_value, upstream, log_decay, segment):
    blocks = N_SEQ
    width = HEAD_COUNT * HEAD

    def project(weight):
        product = jnp.dot(tokens, weight, preferred_element_type=jnp.float32).astype(jnp.bfloat16)
        return product.reshape(blocks, TOK_DEV, HEAD_COUNT, HEAD)
    query = project(w_query)
    key_rows = project(w_key)
    value_rows = project(w_value)
    grads_up = upstream.reshape(blocks, TOK_DEV, HEAD_COUNT, HEAD)
    rates = log_decay.reshape(blocks, TOK_DEV, HEAD_COUNT)
    segs = segment.reshape(blocks, TOK_DEV)
    previous = jnp.concatenate([jnp.full((1,), -1, jnp.int32), segs[:-1, -1]])
    decays, local_states, later_states = lax.map(summaries, (query, key_rows, value_rows, grads_up, rates, segs, previous))

    def forward(state, item):
        decay, segment_state = item
        return (decay[:, None, None] * state + segment_state, state)
    zeros = jnp.zeros((HEAD_COUNT, HEAD, HEAD), jnp.float32)
    _, arriving_state = lax.scan(forward, zeros, (decays, local_states))
    _, backward_state = lax.scan(forward, zeros, (decays, later_states), reverse=True)
    query_gradient, key_gradient, value_gradient = lax.map(block_grads, (query, key_rows, value_rows, grads_up, rates, segs, previous, arriving_state, backward_state))

    def weight_grad(grads):
        flat = grads.reshape(TOKEN_COUNT, width)
        return jnp.dot(tokens.T, flat, preferred_element_type=jnp.float32).astype(jnp.bfloat16)
    return (weight_grad(query_gradient), weight_grad(key_gradient), weight_grad(value_gradient))
```

```python
import functools

import jax
import jax.numpy as jnp
from jax import lax
from jax.experimental import pallas as pl
from jax.experimental.pallas import tpu as pltpu
from jax.sharding import PartitionSpec as P

HEAD = 128
SCALE = HEAD ** (-0.5)
MESH = pl.DeviceIdType.MESH
BF16, F32 = jnp.bfloat16, jnp.float32


def dot(a, b, da, db):
    return lax.dot_general(a, b, (((da,), (db,)), ((), ())), preferred_element_type=F32)


def kernel(
    tok, wq, wk, wv, up, ldt, segv, segs,
    out_q, out_k, out_v,
    x_all, w_all, qkv, qkv_x, upb, up_x, lsb, ct,
    gl, inm, outm, carry, lst, rst, inc, ret, grad, rows_x, rows_r,
    x_recv, x_send, c_recv, c_send, z_recv, z_send, l_recv, l_send, u_recv, u_send,
    g_recv, g_send, d_recv, d_send, o_recv, o_send, loc,
):
    seq, head = lax.axis_index("seq"), lax.axis_index("head")
    z, c = seq // 2, seq % 2
    x, y = head // 4, head % 4
    other = 1 - c

    def at(dz=None, core=None, hx=None, hy=None):
        zz = z if dz is None else dz
        cc = c if core is None else core
        xx = x if hx is None else hx
        yy = y if hy is None else hy
        return {"seq": zz * 2 + cc, "head": xx * 4 + yy}

    xs = [(x + i) % 4 for i in range(4)]
    ys = [(y + i) % 4 for i in range(4)]
    zs = [(z + i) % 8 for i in range(8)]
    partner = at(core=other)
    x_up, x_dn, y_up, y_dn = at(hx=xs[1]), at(hx=xs[3]), at(hy=ys[1]), at(hy=ys[3])
    z_up, z_dn = at(dz=zs[1]), at(dz=zs[7])

    sent = []

    def send(src, dst, ssem, rsem, dev):
        copy = pltpu.make_async_remote_copy(
            src_ref=src, dst_ref=dst, send_sem=ssem, recv_sem=rsem, device_id=dev, device_id_type=MESH
        )
        copy.start()
        sent.append(copy)

    def arrived(dst, ssem, rsem):
        pltpu.make_async_remote_copy(
            src_ref=dst, dst_ref=dst, send_sem=ssem, recv_sem=rsem, device_id=partner, device_id_type=MESH
        ).wait_recv()

    weights = []
    for i, w in enumerate((wq, wk, wv)):
        copy = pltpu.make_async_copy(w, w_all.at[i], loc.at[i])
        copy.start()
        weights.append(copy)
    own_tok = pltpu.make_async_copy(tok, x_all.at[head], loc.at[3])
    own_tok.start()
    own_up = pltpu.make_async_copy(up.at[:, pl.ds(pl.multiple_of(c * 128, 128), 128)], upb.at[seq], loc.at[4])
    own_up.start()
    oth_up = pltpu.make_async_copy(up.at[:, pl.ds(pl.multiple_of(other * 128, 128), 128)], up_x, loc.at[5])
    oth_up.start()

    barrier = pltpu.get_barrier_semaphore()
    near = (partner, x_up, x_dn, y_up, y_dn, z_up, z_dn)
    for dev in near:
        pl.semaphore_signal(barrier, inc=1, device_id=dev, device_id_type=MESH)

    total = jnp.concatenate([ldt[...], jnp.zeros((6, 128), F32)], axis=0)
    lane = lax.broadcasted_iota(jnp.int32, (8, 128), 1)
    for k in (1, 2, 4, 8, 16, 32, 64):
        total = total + jnp.where(lane >= k, pltpu.roll(total, k, 1), 0.0)
    lsb[seq] = total

    own_tok.wait()
    own_up.wait()
    oth_up.wait()
    pl.semaphore_wait(barrier, len(near))

    def plane(unit, recv, sends):
        count = [0]

        def push(ox, oy, half, sub, dev):
            h = ox * 4 + oy
            i = count[0]
            count[0] += 1
            view = unit(h, half, sub)
            send(view, view, sends.at[i], recv.at[half * 2 + (0 if sub is None else sub), h], dev)

        def got(ox, oy, half, sub):
            h = ox * 4 + oy
            view = unit(h, half, sub)
            arrived(view, sends.at[0], recv.at[half * 2 + (0 if sub is None else sub), h])

        def coords(half, first, second):
            return (xs[first], ys[second]) if half == 0 else (xs[second], ys[first])

        def devs(half):
            return ((x_up, x_dn), (y_up, y_dn)) if half == 0 else ((y_up, y_dn), (x_up, x_dn))

        def own():
            for half in (0, 1):
                for dev in devs(half)[0]:
                    push(x, y, half, None, dev)
            for half in (0, 1):
                for dev in devs(half)[1]:
                    push(x, y, half, None, dev)

        def first_near():
            for half in (0, 1):
                (up1, dn1), (up2, dn2) = devs(half)
                ox, oy = coords(half, 3, 0)
                got(ox, oy, half, None)
                push(ox, oy, half, 0, up1)
                push(ox, oy, half, None, up2)
                push(ox, oy, half, None, dn2)
                ox, oy = coords(half, 1, 0)
                got(ox, oy, half, None)
                push(ox, oy, half, 1, dn1)
                push(ox, oy, half, None, up2)
                push(ox, oy, half, None, dn2)

        def second(first):
            def run():
                for half in (0, 1):
                    (up1, dn1), (up2, dn2) = devs(half)
                    ox, oy = coords(half, first, 3)
                    got(ox, oy, half, None)
                    if first in (0, 1):
                        push(ox, oy, half, None, up2)
                    ox, oy = coords(half, first, 1)
                    got(ox, oy, half, None)
                    if first in (2, 3):
                        push(ox, oy, half, None, dn2)
            return run

        def first_far():
            for half in (0, 1):
                (up1, dn1), (up2, dn2) = devs(half)
                ox, oy = coords(half, 2, 0)
                for sub in (0, 1):
                    got(ox, oy, half, sub)
                push(ox, oy, half, None, up2)
                push(ox, oy, half, None, dn2)

        def last():
            for half in (0, 1):
                for first in range(4):
                    ox, oy = coords(half, first, 2)
                    got(ox, oy, half, None)

        return [own, first_near, second(0), second(3), second(1), first_far, second(2), last]

    def x_unit(h, half, sub):
        if sub is None:
            return x_all.at[h, pl.ds(64 * half, 64)]
        return x_all.at[h, pl.ds(64 * half + 32 * sub, 32)]

    def c_unit(h, half, sub):
        cols = pl.ds(pl.multiple_of((h // 8) * 256, 256), 256)
        if sub is None:
            return ct.at[pl.ds(4 * half, 4), c, h % 8, :, cols]
        return ct.at[pl.ds(4 * half + 2 * sub, 2), c, h % 8, :, cols]

    def ring(buf, recv, sends, first_src):
        count = [0]

        def push(src, dst, dev):
            i = count[0]
            count[0] += 1
            send(src, buf.at[dst], sends.at[i], recv.at[dst], dev)

        def got(s):
            arrived(buf.at[s], sends.at[0], recv.at[s])

        def own():
            push(first_src, seq, partner)
            push(buf.at[seq], seq, z_up)
            push(buf.at[seq], seq, z_dn)

        def mate():
            s = z * 2 + other
            got(s)
            push(buf.at[s], s, z_up)
            push(buf.at[s], s, z_dn)

        def hop(d, p):
            def run():
                parity = c if p == 0 else other
                if d < 4:
                    below, above = zs[8 - d] * 2 + parity, zs[d] * 2 + parity
                    got(below)
                    if d < 3 or p == 0:
                        push(buf.at[below], below, z_up)
                    got(above)
                    if d < 3 or p == 1:
                        push(buf.at[above], above, z_dn)
                else:
                    got(zs[4] * 2 + parity)
            return run

        return [own, mate] + [hop(d, p) for d in (1, 2, 3, 4) for p in (0, 1)]

    a_steps = plane(x_unit, x_recv, x_send)
    c_steps = plane(c_unit, c_recv, c_send)
    l_steps = ring(lsb, l_recv, l_send, lsb.at[seq])
    u_steps = ring(upb, u_recv, u_send, up_x)
    g_steps = ring(qkv, g_recv, g_send, qkv_x)

    a_steps[0]()
    l_steps[0]()
    u_steps[0]()
    l_steps[1]()
    u_steps[1]()
    a_steps[1]()
    for i in range(4):
        l_steps[2 + 2 * i]()
        l_steps[3 + 2 * i]()
        u_steps[2 + 2 * i]()
        u_steps[3 + 2 * i]()
        a_steps[2 + i]()
    a_steps[6]()
    a_steps[7]()

    half_h, group = head // 8, head % 8
    cols = pl.ds(pl.multiple_of(half_h * 256, 256), 256)

    def slice_of(zt):
        return x_all.at[2 * zt + half_h, pl.ds(pl.multiple_of(group * 16, 16), 16)]

    own_slice = pltpu.make_async_copy(slice_of(z), ct.at[z, c, group, :, cols], loc.at[6])
    own_slice.start()
    for i in range(1, 8):
        send(slice_of(zs[i]), ct.at[z, c, group, :, cols], z_send.at[i], z_recv.at[z], at(dz=zs[i]))

    for i in range(3):
        weights[i].wait()
    for i in range(3):
        acc = dot(x_all[0], w_all[i, 0:256, :], 1, 0)
        for h in range(1, 16):
            acc = acc + dot(x_all[h], w_all[i, 256 * h : 256 * (h + 1), :], 1, 0)
        acc = acc.astype(BF16)
        qkv[seq, i] = jnp.where(c == 0, acc[:, :128], acc[:, 128:])
        qkv_x[i] = jnp.where(c == 0, acc[:, 128:], acc[:, :128])
    g_steps[0]()

    ti = lax.broadcasted_iota(jnp.int32, (128, 128), 0)
    si = lax.broadcasted_iota(jnp.int32, (128, 128), 1)

    def attend(b):
        q, k, v, u = qkv[b, 0], qkv[b, 1], qkv[b, 2], upb[b]
        sums = lsb[b]
        row = jnp.where(c == 0, sums[0:1], sums[1:2])
        before = segs[jnp.maximum(b * 128 - 1, 0)]
        previous = jnp.where(b > 0, before, -1).astype(F32)
        last = segs[b * 128 + 127].astype(F32)
        ls_s = jnp.broadcast_to(row, (128, 128))
        ls_t = ls_s.T
        seg_s = jnp.broadcast_to(segv[pl.ds(b, 1), :], (128, 128)).astype(F32)
        seg_t = seg_s.T
        same = (seg_s == seg_t) & (ti >= si)
        decay = jnp.where(same, SCALE * jnp.exp(jnp.where(same, ls_t - ls_s, 0.0)), 0.0)
        ls_last = row[:, 127:128]
        inflow = jnp.where(seg_t == previous, jnp.exp(ls_t), 0.0)
        outflow = jnp.where(seg_t == last, jnp.exp(ls_last - ls_t), 0.0)
        keep = jnp.where(last == previous, jnp.exp(ls_last), 0.0)
        carry[b] = jnp.broadcast_to(keep, (8, 128))
        inm[b] = inflow
        outm[b] = outflow
        a_qk = (decay * dot(q, k, 1, 1)).astype(BF16)
        a_up = (decay * dot(u, v, 1, 1)).astype(BF16)
        gl[b, 0] = dot(a_up, k, 1, 0)
        gl[b, 1] = dot(a_up, q, 0, 0)
        gl[b, 2] = dot(a_qk, u, 0, 0)
        wk_ = (SCALE * outflow * k.astype(F32)).astype(BF16)
        wq_ = (SCALE * inflow * q.astype(F32)).astype(BF16)
        lst[b] = dot(wk_, v, 0, 0)
        rst[b] = dot(wq_, u, 0, 0)

    def c_local():
        own_slice.wait()
        for i in range(1, 8):
            arrived(ct.at[zs[i], c, group, :, cols], z_send.at[0], z_recv.at[zs[i]])

    def c_share():
        for i in range(4):
            view = ct.at[pl.ds(2 * i, 2), c]
            send(view, view, d_send.at[i], d_recv.at[i], partner)

    side = [c_local] + c_steps + [c_share]

    g_steps[1]()
    side.pop(0)()
    side.pop(0)()

    def pair(b0, b1):
        def body(i, carry_):
            attend(jnp.where(i == 0, b0, b1))
            return carry_
        lax.fori_loop(0, 2, body, 0)

    pair(seq, z * 2 + other)
    for d in (1, 2, 3):
        for p in (0, 1):
            g_steps[2 + 2 * (d - 1) + p]()
            parity = c if p == 0 else other
            pair(zs[8 - d] * 2 + parity, zs[d] * 2 + parity)
            if side:
                side.pop(0)()
            if side and d == 2:
                side.pop(0)()
    while side:
        side.pop(0)()
    g_steps[8]()
    g_steps[9]()
    pair(zs[4] * 2, zs[4] * 2 + 1)
    for i in range(4):
        arrived(ct.at[pl.ds(2 * i, 2), other], d_send.at[0], d_recv.at[i])

    def forward(b, state):
        inc[b] = state.astype(BF16)
        return carry[b][0:1] * state + lst[b]

    lax.fori_loop(0, 16, forward, jnp.zeros((128, 128), F32))

    def backward(i, state):
        b = 15 - i
        ret[b] = state.astype(BF16)
        return carry[b][0:1] * state + rst[b]

    lax.fori_loop(0, 16, backward, jnp.zeros((128, 128), F32))

    def finish(b, carry_):
        inflow, outflow = inm[b], outm[b]
        grad[b, :, 0:128] = (gl[b, 0] + inflow * dot(upb[b], inc[b], 1, 1)).astype(BF16)
        grad[b, :, 128:256] = (gl[b, 1] + outflow * dot(qkv[b, 2], ret[b], 1, 1)).astype(BF16)
        grad[b, :, 256:384] = (gl[b, 2] + outflow * dot(qkv[b, 1], ret[b], 1, 0)).astype(BF16)
        return carry_

    lax.fori_loop(0, 16, finish, 0)

    def rows_of(core):
        left = ct[:, :, :, :, pl.ds(pl.multiple_of(core * 256, 256), 256)].reshape(2048, 256)
        return dot(left, grad[...].reshape(2048, 384), 0, 0).astype(BF16)

    rows_x[...] = rows_of(other)
    send(rows_x, rows_r, o_send.at[0], o_recv.at[0], partner)
    mine = rows_of(c)
    arrived(rows_r, o_send.at[0], o_recv.at[0])
    theirs = rows_r[...]
    for i, out in enumerate((out_q, out_k, out_v)):
        a, b = mine[:, 128 * i : 128 * (i + 1)], theirs[:, 128 * i : 128 * (i + 1)]
        out[:, 0:128] = jnp.where(c == 0, a, b)
        out[:, 128:256] = jnp.where(c == 0, b, a)
    for copy in sent:
        copy.wait_send()


def local(tokens, w_query, w_key, w_value, upstream, log_decay, segment):
    anyspace = pl.BlockSpec(memory_space=pl.ANY)
    vmem = pl.BlockSpec(memory_space=pltpu.VMEM)
    smem = pl.BlockSpec(memory_space=pltpu.SMEM)
    dma = pltpu.SemaphoreType.DMA
    out = jax.ShapeDtypeStruct((256, 256), BF16)
    return pl.pallas_call(
        kernel,
        out_shape=(out, out, out),
        in_specs=[anyspace] * 5 + [vmem, vmem, smem],
        out_specs=(vmem, vmem, vmem),
        scratch_shapes=[
            pltpu.VMEM((16, 128, 256), BF16),
            pltpu.VMEM((3, 4096, 256), BF16),
            pltpu.VMEM((16, 3, 128, 128), BF16),
            pltpu.VMEM((3, 128, 128), BF16),
            pltpu.VMEM((16, 128, 128), BF16),
            pltpu.VMEM((128, 128), BF16),
            pltpu.VMEM((16, 8, 128), F32),
            pltpu.VMEM((8, 2, 8, 16, 512), BF16),
            pltpu.VMEM((16, 3, 128, 128), F32),
            pltpu.VMEM((16, 128, 128), F32),
            pltpu.VMEM((16, 128, 128), F32),
            pltpu.VMEM((16, 8, 128), F32),
            pltpu.VMEM((16, 128, 128), F32),
            pltpu.VMEM((16, 128, 128), F32),
            pltpu.VMEM((16, 128, 128), BF16),
            pltpu.VMEM((16, 128, 128), BF16),
            pltpu.VMEM((16, 128, 384), BF16),
            pltpu.VMEM((256, 384), BF16),
            pltpu.VMEM((256, 384), BF16),
            dma((4, 16)), dma((32,)),
            dma((4, 16)), dma((32,)),
            dma((8,)), dma((8,)),
            dma((16,)), dma((15,)),
            dma((16,)), dma((15,)),
            dma((16,)), dma((15,)),
            dma((4,)), dma((4,)),
            dma((1,)), dma((1,)),
            dma((7,)),
        ],
        compiler_params=pltpu.CompilerParams(
            collective_id=0, has_side_effects=True, vmem_limit_bytes=60 * 1024 * 1024
        ),
    )(
        tokens, w_query, w_key, w_value, upstream,
        log_decay.T, segment.reshape(16, 128), segment,
    )


def solution(mesh):
    in_specs = (
        P("seq", "head"), P(None, "head"), P(None, "head"), P(None, "head"),
        P("seq", "head"), P("seq", "head"), P(),
    )
    out_specs = (P("seq", "head"),) * 3
    return jax.shard_map(local, mesh=mesh, in_specs=in_specs, out_specs=out_specs, check_vma=False)
```

```python
import functools

import jax
import jax.numpy as jnp
from jax import lax
from jax.experimental import pallas as pl
from jax.experimental.pallas import tpu as pltpu
from jax.sharding import PartitionSpec as P

HEAD = 128
SCALE = HEAD ** (-0.5)
MESH = pl.DeviceIdType.MESH
BF16, F32 = jnp.bfloat16, jnp.float32


def dot(a, b, da, db):
    return lax.dot_general(a, b, (((da,), (db,)), ((), ())), preferred_element_type=F32)


def kernel(
    tok, wq, wk, wv, up, ldt_in, segv_in, segs_in,
    out,
    ldt, segv, segs, x_all, w_all, qkv, qkv_x, upb, up_x, ct,
    gl, inm, outm, carry, lst, rst, inc, ret, grad, rows_x, rows_r,
    x_recv, x_send, c_recv, c_send, z_recv, z_send, u_recv, u_send,
    g_recv, g_send, d_recv, d_send, o_recv, o_send, loc,
):
    seq, head = lax.axis_index("seq"), lax.axis_index("head")
    z, c = seq // 2, seq % 2
    x, y = head // 4, head % 4
    other = 1 - c

    def at(dz=None, core=None, hx=None, hy=None):
        zz = z if dz is None else dz
        cc = c if core is None else core
        xx = x if hx is None else hx
        yy = y if hy is None else hy
        return {"seq": zz * 2 + cc, "head": xx * 4 + yy}

    xs = [(x + i) % 4 for i in range(4)]
    ys = [(y + i) % 4 for i in range(4)]
    zs = [(z + i) % 8 for i in range(8)]
    partner = at(core=other)
    x_up, x_dn, y_up, y_dn = at(hx=xs[1]), at(hx=xs[3]), at(hy=ys[1]), at(hy=ys[3])
    z_up, z_dn = at(dz=zs[1]), at(dz=zs[7])

    sent = []

    def send(src, dst, ssem, rsem, dev):
        copy = pltpu.make_async_remote_copy(
            src_ref=src, dst_ref=dst, send_sem=ssem, recv_sem=rsem, device_id=dev, device_id_type=MESH
        )
        copy.start()
        sent.append(copy)

    def arrived(dst, ssem, rsem):
        pltpu.make_async_remote_copy(
            src_ref=dst, dst_ref=dst, send_sem=ssem, recv_sem=rsem, device_id=partner, device_id_type=MESH
        ).wait_recv()

    barrier = pltpu.get_barrier_semaphore()
    near = [partner, x_up, x_dn, y_up, y_dn] + [at(dz=zs[i]) for i in range(1, 8)]
    for dev in near:
        pl.semaphore_signal(barrier, inc=1, device_id=dev, device_id_type=MESH)

    def fetch(src, dst, i):
        copy = pltpu.make_async_copy(src, dst, loc.at[i])
        copy.start()
        return copy

    def lanes(i):
        return pl.ds(pl.multiple_of(i * 128, 128), 128)

    own_tok = fetch(tok, x_all.at[head], 0)
    own_ldt = fetch(ldt_in, ldt, 1)
    own_up = fetch(up.at[:, lanes(c)], upb.at[seq, 0:128], 2)
    oth_up = fetch(up.at[:, lanes(other)], up_x.at[0:128], 3)
    seg_v = fetch(segv_in, segv, 4)
    seg_s = fetch(segs_in, segs, 5)
    weights = [fetch(w, w_all.at[i], 7 + i) for i, w in enumerate((wq, wk, wv))]

    own_ldt.wait()
    total = jnp.concatenate([ldt[...], jnp.zeros((6, 128), F32)], axis=0)
    lane = lax.broadcasted_iota(jnp.int32, (8, 128), 1)
    for k in (1, 2, 4, 8, 16, 32, 64):
        total = total + jnp.where(lane >= k, pltpu.roll(total, k, 1), 0.0)

    def in_parts(row):
        hi = row.astype(BF16)
        rest = row - hi.astype(F32)
        mid = rest.astype(BF16)
        low = (rest - mid.astype(F32)).astype(BF16)
        return jnp.concatenate([hi.astype(F32), mid.astype(F32), low.astype(F32), jnp.zeros((13, 128), F32)], axis=0).astype(BF16)

    lo, hi = in_parts(total[0:1]), in_parts(total[1:2])
    upb[seq, 128:144] = jnp.where(c == 0, lo, hi)
    up_x[128:144] = jnp.where(c == 0, hi, lo)

    own_tok.wait()
    pl.semaphore_wait(barrier, len(near))

    def plane(unit, recv, sends):
        count = [0]

        def push(ox, oy, half, sub, dev):
            h = ox * 4 + oy
            i = count[0]
            count[0] += 1
            view = unit(h, half, sub)
            send(view, view, sends.at[i], recv.at[half * 2 + (0 if sub is None else sub), h], dev)

        def got(ox, oy, half, sub):
            h = ox * 4 + oy
            view = unit(h, half, sub)
            arrived(view, sends.at[0], recv.at[half * 2 + (0 if sub is None else sub), h])

        def coords(half, first, second):
            return (xs[first], ys[second]) if half == 0 else (xs[second], ys[first])

        def devs(half):
            return ((x_up, x_dn), (y_up, y_dn)) if half == 0 else ((y_up, y_dn), (x_up, x_dn))

        def own():
            for half in (0, 1):
                for dev in devs(half)[0]:
                    push(x, y, half, None, dev)
            for half in (0, 1):
                for dev in devs(half)[1]:
                    push(x, y, half, None, dev)

        def first_near():
            for half in (0, 1):
                (up1, dn1), (up2, dn2) = devs(half)
                ox, oy = coords(half, 3, 0)
                got(ox, oy, half, None)
                push(ox, oy, half, 0, up1)
                push(ox, oy, half, None, up2)
                push(ox, oy, half, None, dn2)
                ox, oy = coords(half, 1, 0)
                got(ox, oy, half, None)
                push(ox, oy, half, 1, dn1)
                push(ox, oy, half, None, up2)
                push(ox, oy, half, None, dn2)

        def second(first):
            def run():
                for half in (0, 1):
                    (up1, dn1), (up2, dn2) = devs(half)
                    ox, oy = coords(half, first, 3)
                    got(ox, oy, half, None)
                    if first in (0, 1):
                        push(ox, oy, half, None, up2)
                    ox, oy = coords(half, first, 1)
                    got(ox, oy, half, None)
                    if first in (2, 3):
                        push(ox, oy, half, None, dn2)
            return run

        def first_far():
            for half in (0, 1):
                (up1, dn1), (up2, dn2) = devs(half)
                ox, oy = coords(half, 2, 0)
                for sub in (0, 1):
                    got(ox, oy, half, sub)
                push(ox, oy, half, None, up2)
                push(ox, oy, half, None, dn2)

        def last(first):
            def run():
                for half in (0, 1):
                    ox, oy = coords(half, first, 2)
                    got(ox, oy, half, None)
            return run

        return [
            [own],
            [first_near, second(0)],
            [first_far, second(3), second(1), last(0)],
            [second(2), last(1), last(3)],
            [last(2)],
        ]

    def x_unit(h, half, sub):
        if sub is None:
            return x_all.at[h, pl.ds(64 * half, 64)]
        return x_all.at[h, pl.ds(64 * half + 32 * sub, 32)]

    def c_unit(h, half, sub):
        if sub is None:
            return ct.at[h // 8, pl.ds(4 * half, 4), c, h % 8]
        return ct.at[h // 8, pl.ds(4 * half + 2 * sub, 2), c, h % 8]

    def ring(buf, recv, sends, first_src):
        count = [0]

        def push(src, dst, dev):
            i = count[0]
            count[0] += 1
            send(src, buf.at[dst], sends.at[i], recv.at[dst], dev)

        def got(s):
            arrived(buf.at[s], sends.at[0], recv.at[s])

        def own():
            push(first_src, seq, partner)
            push(buf.at[seq], seq, z_up)
            push(buf.at[seq], seq, z_dn)

        def mate():
            s = z * 2 + other
            got(s)
            push(buf.at[s], s, z_up)
            push(buf.at[s], s, z_dn)

        def hop(d, p):
            def run():
                parity = c if p == 0 else other
                if d < 4:
                    below, above = zs[8 - d] * 2 + parity, zs[d] * 2 + parity
                    got(below)
                    if d < 3 or p == 0:
                        push(buf.at[below], below, z_up)
                    got(above)
                    if d < 3 or p == 1:
                        push(buf.at[above], above, z_dn)
                else:
                    got(zs[4] * 2 + parity)
            return run

        return [own, mate] + [hop(d, p) for d in (1, 2, 3, 4) for p in (0, 1)]

    a_steps = plane(x_unit, x_recv, x_send)
    c_steps = plane(c_unit, c_recv, c_send)
    u_steps = ring(upb, u_recv, u_send, up_x)
    g_steps = ring(qkv, g_recv, g_send, qkv_x)

    def run(steps):
        for step in steps:
            step()

    run(a_steps[0])
    own_up.wait()
    oth_up.wait()
    run(u_steps[0:2])
    run(a_steps[1])
    run(u_steps[2:4])
    run(a_steps[2])
    run(u_steps[4:6])
    run(a_steps[3])
    run(a_steps[4])

    half_h, group = head // 8, head % 8

    def slice_of(zt):
        return x_all.at[2 * zt + half_h, pl.ds(pl.multiple_of(group * 16, 16), 16)]

    own_slice = pltpu.make_async_copy(slice_of(z), ct.at[half_h, z, c, group], loc.at[6])
    own_slice.start()
    for i in range(1, 8):
        send(slice_of(zs[i]), ct.at[half_h, z, c, group], z_send.at[i], z_recv.at[z], at(dz=zs[i]))

    for copy in weights:
        copy.wait()
    seg_v.wait()
    seg_s.wait()
    for i in range(3):
        acc = dot(x_all[0], w_all[i, 0:256, :], 1, 0)
        for h in range(1, 16):
            acc = acc + dot(x_all[h], w_all[i, 256 * h : 256 * (h + 1), :], 1, 0)
        acc = acc.astype(BF16)
        qkv[seq, i] = jnp.where(c == 0, acc[:, :128], acc[:, 128:])
        qkv_x[i] = jnp.where(c == 0, acc[:, 128:], acc[:, :128])
    g_steps[0]()
    run(u_steps[6:8])
    g_steps[1]()

    ti = lax.broadcasted_iota(jnp.int32, (128, 128), 0)
    si = lax.broadcasted_iota(jnp.int32, (128, 128), 1)

    def attend(blocks):
        done = []
        for b in blocks:
            q, k, v, u = qkv[b, 0], qkv[b, 1], qkv[b, 2], upb[b, 0:128]
            parts = upb[b, 128:144].astype(F32)
            row = parts[0:1] + parts[1:2] + parts[2:3]
            before = segs[jnp.maximum(b * 128 - 1, 0)]
            previous = jnp.where(b > 0, before, -1).astype(F32)
            last = segs[b * 128 + 127].astype(F32)
            ls_s = jnp.broadcast_to(row, (128, 128))
            ls_t = ls_s.T
            seg_s = jnp.broadcast_to(segv[pl.ds(b, 1), :], (128, 128)).astype(F32)
            seg_t = seg_s.T
            same = (seg_s == seg_t) & (ti >= si)
            decay = jnp.where(same, SCALE * jnp.exp(jnp.where(same, ls_t - ls_s, 0.0)), 0.0)
            ls_last = row[:, 127:128]
            inflow = jnp.where(seg_t == previous, jnp.exp(ls_t), 0.0)
            outflow = jnp.where(seg_t == last, jnp.exp(ls_last - ls_t), 0.0)
            keep = jnp.where(last == previous, jnp.exp(ls_last), 0.0)
            a_qk = (decay * dot(q, k, 1, 1)).astype(BF16)
            a_up = (decay * dot(u, v, 1, 1)).astype(BF16)
            wk_ = (SCALE * outflow * k.astype(F32)).astype(BF16)
            wq_ = (SCALE * inflow * q.astype(F32)).astype(BF16)
            done.append((
                inflow, outflow, jnp.broadcast_to(keep, (8, 128)), dot(a_up, k, 1, 0), dot(a_up, q, 0, 0),
                dot(a_qk, u, 0, 0), dot(wk_, v, 0, 0), dot(wq_, u, 0, 0),
            ))
        for b, (inflow, outflow, keep, gq, gk, gv, ls, rs) in zip(blocks, done):
            inm[b], outm[b], carry[b] = inflow, outflow, keep
            gl[b, 0], gl[b, 1], gl[b, 2] = gq, gk, gv
            lst[b], rst[b] = ls, rs

    def c_local():
        own_slice.wait()
        for i in range(1, 8):
            arrived(ct.at[half_h, zs[i], c, group], z_send.at[0], z_recv.at[zs[i]])

    def c_share():
        for i in range(4):
            view = ct.at[:, pl.ds(2 * i, 2), c]
            send(view, view, d_send.at[i], d_recv.at[i], partner)

    side = [[c_local] + c_steps[0]] + c_steps[1:] + [[c_share]]

    attend((seq, z * 2 + other))
    run(side[0])
    n = 1
    for d in (1, 2, 3):
        for p in (0, 1):
            g_steps[2 + 2 * (d - 1) + p]()
            parity = c if p == 0 else other
            attend((zs[8 - d] * 2 + parity, zs[d] * 2 + parity))
            if n < len(side):
                run(side[n])
                n += 1
            if d == 1 and p == 1:
                run(u_steps[8:10])
    for i in range(4):
        arrived(ct.at[:, pl.ds(2 * i, 2), other], d_send.at[0], d_recv.at[i])
    g_steps[8]()
    g_steps[9]()
    attend((zs[4] * 2, zs[4] * 2 + 1))

    def forward(b, state):
        inc[b] = state.astype(BF16)
        return carry[b][0:1] * state + lst[b]

    lax.fori_loop(0, 16, forward, jnp.zeros((128, 128), F32))

    def backward(i, state):
        b = 15 - i
        ret[b] = state.astype(BF16)
        return carry[b][0:1] * state + rst[b]

    lax.fori_loop(0, 16, backward, jnp.zeros((128, 128), F32))

    def finish(i, carry_):
        done = []
        for b in (4 * i, 4 * i + 1, 4 * i + 2, 4 * i + 3):
            inflow, outflow = inm[b], outm[b]
            done.append((
                gl[b, 0] + inflow * dot(upb[b, 0:128], inc[b], 1, 1),
                gl[b, 1] + outflow * dot(qkv[b, 2], ret[b], 1, 1),
                gl[b, 2] + outflow * dot(qkv[b, 1], ret[b], 1, 0),
            ))
        for j, parts in enumerate(done):
            for k, part in enumerate(parts):
                grad[4 * i + j, :, 128 * k : 128 * (k + 1)] = part.astype(BF16)
        return carry_

    lax.fori_loop(0, 4, finish, 0)

    def rows_of(core):
        return dot(ct[core].reshape(2048, 256), grad[...].reshape(2048, 384), 0, 0).astype(BF16)

    rows_x[...] = rows_of(other)
    send(rows_x, rows_r, o_send.at[0], o_recv.at[0], partner)
    mine = rows_of(c)
    for i in range(3):
        out[i, :, lanes(c)] = mine[:, 128 * i : 128 * (i + 1)]
    arrived(rows_r, o_send.at[0], o_recv.at[0])
    for i in range(3):
        out[i, :, lanes(other)] = rows_r[:, 128 * i : 128 * (i + 1)]
    for copy in sent:
        copy.wait_send()


def local(tokens, w_query, w_key, w_value, upstream, log_decay, segment):
    hbm = pl.BlockSpec(memory_space=pltpu.HBM)
    dma = pltpu.SemaphoreType.DMA
    out = pl.pallas_call(
        kernel,
        out_shape=jax.ShapeDtypeStruct((3, 256, 256), BF16),
        in_specs=[hbm] * 8,
        out_specs=pl.BlockSpec(memory_space=pltpu.VMEM),
        scratch_shapes=[
            pltpu.VMEM((2, 128), F32),
            pltpu.VMEM((16, 128), jnp.int32),
            pltpu.SMEM((2048,), jnp.int32),
            pltpu.VMEM((16, 128, 256), BF16),
            pltpu.VMEM((3, 4096, 256), BF16),
            pltpu.VMEM((16, 3, 128, 128), BF16),
            pltpu.VMEM((3, 128, 128), BF16),
            pltpu.VMEM((16, 144, 128), BF16),
            pltpu.VMEM((144, 128), BF16),
            pltpu.VMEM((2, 8, 2, 8, 16, 256), BF16),
            pltpu.VMEM((16, 3, 128, 128), F32),
            pltpu.VMEM((16, 128, 128), F32),
            pltpu.VMEM((16, 128, 128), F32),
            pltpu.VMEM((16, 8, 128), F32),
            pltpu.VMEM((16, 128, 128), F32),
            pltpu.VMEM((16, 128, 128), F32),
            pltpu.VMEM((16, 128, 128), BF16),
            pltpu.VMEM((16, 128, 128), BF16),
            pltpu.VMEM((16, 128, 384), BF16),
            pltpu.VMEM((256, 384), BF16),
            pltpu.VMEM((256, 384), BF16),
            dma((4, 16)), dma((32,)),
            dma((4, 16)), dma((32,)),
            dma((8,)), dma((8,)),
            dma((16,)), dma((15,)),
            dma((16,)), dma((15,)),
            dma((4,)), dma((4,)),
            dma((1,)), dma((1,)),
            dma((10,)),
        ],
        compiler_params=pltpu.CompilerParams(
            collective_id=0, has_side_effects=True, vmem_limit_bytes=60 * 1024 * 1024
        ),
    )(
        tokens, w_query, w_key, w_value, upstream,
        log_decay.T, segment.reshape(16, 128), segment,
    )
    return out[0], out[1], out[2]


def solution(mesh):
    in_specs = (
        P("seq", "head"), P(None, "head"), P(None, "head"), P(None, "head"),
        P("seq", "head"), P("seq", "head"), P(),
    )
    out_specs = (P("seq", "head"),) * 3
    return jax.shard_map(local, mesh=mesh, in_specs=in_specs, out_specs=out_specs, check_vma=False)
```

```python
import jax
import jax.numpy as jnp
from jax import lax
from jax.experimental import pallas as pl
from jax.experimental.pallas import tpu as pltpu
from jax.sharding import PartitionSpec as P

HEAD = 128
SCALE = HEAD ** (-0.5)
MESH = pl.DeviceIdType.MESH
BF16, F32 = jnp.bfloat16, jnp.float32
AROUND = (1, 3, 2)


def dot(a, b, da, db):
    return lax.dot_general(a, b, (((da,), (db,)), ((), ())), preferred_element_type=F32)


def kernel(
    tok, wq, wk, wv, up, ldt_in, segv_in, segs_in,
    out,
    ldt, segv, segs, x_all, w_all, qkv, qkv_x, upb, up_x, ct,
    gl, inm, outm, carry, lst, rst, inc, ret, grad, rows_x, rows_r,
    x_first, x_rest, c_first, c_rest, z_recv, u_recv, g_mate, g_recv, d_recv, o_recv, sends, loc,
):
    seq, head = lax.axis_index("seq"), lax.axis_index("head")
    z, c = seq // 2, seq % 2
    x, y = head // 4, head % 4
    other = 1 - c
    zs = [(z + i) % 8 for i in range(8)]

    def plane_at(dx, dy):
        return ((x + dx) % 4) * 4 + (y + dy) % 4

    def at(dz=0, dx=0, dy=0, core=None):
        return {"seq": zs[dz] * 2 + (c if core is None else core), "head": plane_at(dx, dy)}

    partner = at(core=other)
    barrier = pltpu.get_barrier_semaphore()
    near = [partner] + [at(dx=i) for i in AROUND] + [at(dy=i) for i in AROUND] + [at(dz=i) for i in range(1, 8)]
    for dev in near:
        pl.semaphore_signal(barrier, inc=1, device_id=dev, device_id_type=MESH)

    def fetch(src, dst, i):
        copy = pltpu.make_async_copy(src, dst, loc.at[i])
        copy.start()
        return copy

    def lanes(i):
        return pl.ds(pl.multiple_of(i * 128, 128), 128)

    own_tok = [fetch(tok.at[:, 128 * i : 128 * (i + 1)], x_all.at[i, head], i) for i in range(2)]
    own_ldt = fetch(ldt_in, ldt, 2)
    own_up = fetch(up.at[:, lanes(c)], upb.at[seq, 0:128], 3)
    oth_up = fetch(up.at[:, lanes(other)], up_x.at[0:128], 4)
    seg_v = fetch(segv_in, segv, 5)
    seg_s = fetch(segs_in, segs, 6)
    weights = [fetch(w, w_all.at[i], 7 + i) for i, w in enumerate((wq, wk, wv))]

    own_ldt.wait()
    total = jnp.concatenate([ldt[...], jnp.zeros((6, 128), F32)], axis=0)
    lane = lax.broadcasted_iota(jnp.int32, (8, 128), 1)
    for k in (1, 2, 4, 8, 16, 32, 64):
        total = total + jnp.where(lane >= k, pltpu.roll(total, k, 1), 0.0)

    def in_parts(row):
        hi = row.astype(BF16)
        rest = row - hi.astype(F32)
        mid = rest.astype(BF16)
        low = (rest - mid.astype(F32)).astype(BF16)
        return jnp.concatenate([hi.astype(F32), mid.astype(F32), low.astype(F32), jnp.zeros((13, 128), F32)], axis=0).astype(BF16)

    lo, hi = in_parts(total[0:1]), in_parts(total[1:2])
    upb[seq, 128:144] = jnp.where(c == 0, lo, hi)
    up_x[128:144] = jnp.where(c == 0, hi, lo)

    for copy in own_tok:
        copy.wait()
    pl.semaphore_wait(barrier, len(near))

    sent = {}

    def send(kind, src, dst, recv, dev):
        rows = src.dtype.itemsize
        for n in src.shape:
            rows *= n
        sent[kind] = sent.get(kind, 0) + rows // 512
        pltpu.make_async_remote_copy(
            src_ref=src, dst_ref=dst, send_sem=sends.at[kind], recv_sem=recv, device_id=dev, device_id_type=MESH
        ).start()

    def described(view, recv):
        return pltpu.make_async_remote_copy(
            src_ref=view, dst_ref=view, send_sem=sends.at[0], recv_sem=recv, device_id=partner, device_id_type=MESH
        )

    def arrived(view, recv):
        described(view, recv).wait_recv()

    def arrived_rows(rows, recv):
        arrived(w_all.at[0, 0:rows], recv)

    def plane(kind, unit, rows, first, rest):
        def there(half, stage, d):
            return at(dx=d) if half == stage else at(dy=d)

        def own():
            for half in (0, 1):
                for j, d in enumerate(AROUND):
                    view = unit(head, half)
                    send(kind, view, view, first.at[half, j], there(half, 0, d))
            for half in (0, 1):
                for d in AROUND:
                    view = unit(head, half)
                    send(kind, view, view, rest, there(half, 1, d))

        def middle():
            for j, d in enumerate(AROUND):
                for half in (0, 1):
                    view = unit(plane_at(-d, 0) if half == 0 else plane_at(0, -d), half)
                    arrived(view, first.at[half, j])
                    for e in AROUND:
                        send(kind, view, view, rest, there(half, 1, e))

        def end():
            arrived_rows(24 * rows, rest)

        return own, middle, end

    def x_unit(k):
        return lambda h, half: x_all.at[half, h, 64 * k : 64 * (k + 1)]

    def c_unit(h, half):
        return ct.at[h // 8, (h // 4) % 2, 4 * half : 4 * (half + 1), c, h % 4]

    def up_own():
        send(2, up_x, upb.at[seq], u_recv.at[8], partner)
        send(2, upb.at[seq], upb.at[seq], u_recv.at[0], at(dz=1))
        send(2, upb.at[seq], upb.at[seq], u_recv.at[4], at(dz=7))

    def up_mate():
        s = z * 2 + other
        arrived(upb.at[s], u_recv.at[8])
        send(2, upb.at[s], upb.at[s], u_recv.at[0], at(dz=1))
        send(2, upb.at[s], upb.at[s], u_recv.at[4], at(dz=7))

    def up_hop(d):
        below, above = zs[8 - d] * 2, zs[d] * 2
        count = 2 if d < 4 else 1
        arrived(upb.at[0:count], u_recv.at[d - 1])
        if d < 4:
            for parity in (c, other) if d < 3 else (c,):
                send(2, upb.at[below + parity], upb.at[below + parity], u_recv.at[d], at(dz=1))
        arrived(upb.at[0:count], u_recv.at[4 + d - 1])
        if d < 4:
            for parity in (c, other) if d < 3 else (other,):
                send(2, upb.at[above + parity], upb.at[above + parity], u_recv.at[4 + d], at(dz=7))

    def g_to_next(s, p, k, d, both=True, down=False):
        view = qkv.at[s, k]
        if both or not down:
            send(3, view, view, g_recv.at[((0 * 4 + d) * 2 + p) * 2 + k], at(dz=1))
        if both or down:
            send(3, view, view, g_recv.at[((1 * 4 + d) * 2 + p) * 2 + k], at(dz=7))

    def g_own(k):
        send(3, qkv_x.at[k], qkv.at[seq, k], g_mate.at[k], partner)
        g_to_next(seq, 0, k, 0)

    def g_from_mate(k):
        s = z * 2 + other
        arrived(qkv.at[s, k], g_mate.at[k])
        g_to_next(s, 1, k, 0)

    def g_hop(d, p, k):
        parity = c if p == 0 else other
        if d < 4 or p == 0:
            s = zs[8 - d] * 2 + parity
            arrived(qkv.at[s, k], g_recv.at[((0 * 4 + d - 1) * 2 + p) * 2 + k])
            if d < 3 or (d == 3 and p == 0):
                g_to_next(s, p, k, d, both=False)
        if d < 4 or p == 1:
            s = zs[d] * 2 + parity
            arrived(qkv.at[s, k], g_recv.at[((1 * 4 + d - 1) * 2 + p) * 2 + k])
            if d < 3 or (d == 3 and p == 1):
                g_to_next(s, p, k, d, both=False, down=True)

    def project(k):
        for i in range(3):
            acc = jnp.zeros((64, 256), F32)
            for h in range(16):
                left = jnp.concatenate([x_all[j, h, 64 * k : 64 * (k + 1)] for j in (0, 1)], axis=1)
                acc = acc + dot(left, w_all[i, 256 * h : 256 * (h + 1), :], 1, 0)
            acc = acc.astype(BF16)
            qkv[seq, k, i] = jnp.where(c == 0, acc[:, :128], acc[:, 128:])
            qkv_x[k, i] = jnp.where(c == 0, acc[:, 128:], acc[:, :128])

    a_own, a_mid, a_end = zip(*[plane(0, x_unit(k), 32, x_first.at[k], x_rest.at[k]) for k in (0, 1)])
    c_own, c_mid, c_end = plane(1, c_unit, 64, c_first, c_rest)

    a_own[0]()
    a_own[1]()
    own_up.wait()
    oth_up.wait()
    up_own()
    up_mate()
    a_mid[0]()
    a_mid[1]()
    up_hop(1)
    for copy in weights:
        copy.wait()
    seg_v.wait()
    seg_s.wait()
    a_end[0]()
    project(0)
    g_own(0)
    g_from_mate(0)
    up_hop(2)
    a_end[1]()

    f, hb, rg = head // 8, (head // 4) % 2, head % 4

    def slice_of(zt):
        return x_all.at[hb, 2 * zt + f, pl.ds(pl.multiple_of(rg * 32, 32), 32)]

    own_slice = fetch(slice_of(z), ct.at[f, hb, z, c, rg], 0)
    for i in range(1, 8):
        send(4, slice_of(zs[i]), ct.at[f, hb, z, c, rg], z_recv.at[0], at(dz=i))
    project(1)
    g_own(1)
    g_from_mate(1)
    up_hop(3)

    ti = lax.broadcasted_iota(jnp.int32, (128, 128), 0)
    si = lax.broadcasted_iota(jnp.int32, (128, 128), 1)

    def part(b, i):
        return jnp.concatenate([qkv[b, 0, i], qkv[b, 1, i]], axis=0)

    def attend(blocks):
        done = []
        for b in blocks:
            q, k, v, u = part(b, 0), part(b, 1), part(b, 2), upb[b, 0:128]
            parts = upb[b, 128:144].astype(F32)
            row = parts[0:1] + parts[1:2] + parts[2:3]
            before = segs[jnp.maximum(b * 128 - 1, 0)]
            previous = jnp.where(b > 0, before, -1).astype(F32)
            last = segs[b * 128 + 127].astype(F32)
            ls_s = jnp.broadcast_to(row, (128, 128))
            ls_t = ls_s.T
            seg_s = jnp.broadcast_to(segv[pl.ds(b, 1), :], (128, 128)).astype(F32)
            seg_t = seg_s.T
            same = (seg_s == seg_t) & (ti >= si)
            decay = jnp.where(same, SCALE * jnp.exp(jnp.where(same, ls_t - ls_s, 0.0)), 0.0)
            ls_last = row[:, 127:128]
            inflow = jnp.where(seg_t == previous, jnp.exp(ls_t), 0.0)
            outflow = jnp.where(seg_t == last, jnp.exp(ls_last - ls_t), 0.0)
            keep = jnp.where(last == previous, jnp.exp(ls_last), 0.0)
            a_qk = (decay * dot(q, k, 1, 1)).astype(BF16)
            a_up = (decay * dot(u, v, 1, 1)).astype(BF16)
            wk_ = (SCALE * outflow * k.astype(F32)).astype(BF16)
            wq_ = (SCALE * inflow * q.astype(F32)).astype(BF16)
            done.append((
                inflow, outflow, jnp.broadcast_to(keep, (8, 128)), dot(a_up, k, 1, 0), dot(a_up, q, 0, 0),
                dot(a_qk, u, 0, 0), dot(wk_, v, 0, 0), dot(wq_, u, 0, 0),
            ))
        for b, (inflow, outflow, keep, gq, gk, gv, ls, rs) in zip(blocks, done):
            inm[b], outm[b], carry[b] = inflow, outflow, keep
            gl[b, 0], gl[b, 1], gl[b, 2] = gq, gk, gv
            lst[b], rst[b] = ls, rs

    def c_begin():
        own_slice.wait()
        arrived_rows(7 * 16, z_recv.at[0])
        c_own()

    def c_share():
        c_end()
        for i in (0, 1):
            view = ct.at[i, :, :, c]
            send(5, view, view, d_recv.at[i], partner)

    def up_last():
        up_hop(4)

    attend((seq, z * 2 + other))
    side = {(1, 0): c_begin, (1, 1): up_last, (2, 0): c_mid, (3, 1): c_share}
    for d in (1, 2, 3):
        for p in (0, 1):
            parity = c if p == 0 else other
            if p == 0:
                g_hop(d, 0, 0)
                g_hop(d, 1, 0)
            g_hop(d, p, 1)
            attend((zs[8 - d] * 2 + parity, zs[d] * 2 + parity))
            if (d, p) in side:
                side[d, p]()
    for p in (0, 1):
        for k in (0, 1):
            g_hop(4, p, k)
    attend((zs[4] * 2, zs[4] * 2 + 1))

    def forward(b, state):
        inc[b] = state.astype(BF16)
        return carry[b][0:1] * state + lst[b]

    lax.fori_loop(0, 16, forward, jnp.zeros((128, 128), F32))

    def backward(i, state):
        b = 15 - i
        ret[b] = state.astype(BF16)
        return carry[b][0:1] * state + rst[b]

    lax.fori_loop(0, 16, backward, jnp.zeros((128, 128), F32))

    def finish(i, carry_):
        done = []
        for b in (4 * i, 4 * i + 1, 4 * i + 2, 4 * i + 3):
            inflow, outflow = inm[b], outm[b]
            done.append((
                gl[b, 0] + inflow * dot(upb[b, 0:128], inc[b], 1, 1),
                gl[b, 1] + outflow * dot(part(b, 2), ret[b], 1, 1),
                gl[b, 2] + outflow * dot(part(b, 1), ret[b], 1, 0),
            ))
        for j, parts in enumerate(done):
            for k, value in enumerate(parts):
                grad[4 * i + j, :, 128 * k : 128 * (k + 1)] = value.astype(BF16)
        return carry_

    lax.fori_loop(0, 4, finish, 0)
    for i in (0, 1):
        arrived(ct.at[i, :, :, other], d_recv.at[i])

    def rows_of(core):
        left = jnp.concatenate([ct[core, j].reshape(2048, 128) for j in (0, 1)], axis=1)
        return dot(left, grad[...].reshape(2048, 384), 0, 0).astype(BF16)

    rows_x[...] = rows_of(other)
    send(6, rows_x, rows_r, o_recv.at[0], partner)
    mine = rows_of(c)
    for i in range(3):
        out[i, :, lanes(c)] = mine[:, 128 * i : 128 * (i + 1)]
    arrived(rows_r, o_recv.at[0])
    for i in range(3):
        out[i, :, lanes(other)] = rows_r[:, 128 * i : 128 * (i + 1)]
    for kind, rows in sent.items():
        view = w_all.at[0, 0:rows]
        pltpu.make_async_remote_copy(
            src_ref=view, dst_ref=view, send_sem=sends.at[kind], recv_sem=loc.at[0], device_id=partner, device_id_type=MESH
        ).wait_send()


def local(tokens, w_query, w_key, w_value, upstream, log_decay, segment):
    hbm = pl.BlockSpec(memory_space=pltpu.HBM)
    dma = pltpu.SemaphoreType.DMA
    out = pl.pallas_call(
        kernel,
        out_shape=jax.ShapeDtypeStruct((3, 256, 256), BF16),
        in_specs=[hbm] * 8,
        out_specs=pl.BlockSpec(memory_space=pltpu.VMEM),
        scratch_shapes=[
            pltpu.VMEM((2, 128), F32),
            pltpu.VMEM((16, 128), jnp.int32),
            pltpu.SMEM((2048,), jnp.int32),
            pltpu.VMEM((2, 16, 128, 128), BF16),
            pltpu.VMEM((3, 4096, 256), BF16),
            pltpu.VMEM((16, 2, 3, 64, 128), BF16),
            pltpu.VMEM((2, 3, 64, 128), BF16),
            pltpu.VMEM((16, 144, 128), BF16),
            pltpu.VMEM((144, 128), BF16),
            pltpu.VMEM((2, 2, 8, 2, 4, 32, 128), BF16),
            pltpu.VMEM((16, 3, 128, 128), F32),
            pltpu.VMEM((16, 128, 128), F32),
            pltpu.VMEM((16, 128, 128), F32),
            pltpu.VMEM((16, 8, 128), F32),
            pltpu.VMEM((16, 128, 128), F32),
            pltpu.VMEM((16, 128, 128), F32),
            pltpu.VMEM((16, 128, 128), BF16),
            pltpu.VMEM((16, 128, 128), BF16),
            pltpu.VMEM((16, 128, 384), BF16),
            pltpu.VMEM((256, 384), BF16),
            pltpu.VMEM((256, 384), BF16),
            dma((2, 2, 3)), dma((2,)),
            dma((2, 3)), dma(()),
            dma((1,)), dma((9,)),
            dma((2,)), dma((32,)),
            dma((2,)), dma((1,)),
            dma((7,)), dma((10,)),
        ],
        compiler_params=pltpu.CompilerParams(
            collective_id=0, has_side_effects=True, vmem_limit_bytes=60 * 1024 * 1024
        ),
    )(
        tokens, w_query, w_key, w_value, upstream,
        log_decay.T, segment.reshape(16, 128), segment,
    )
    return out[0], out[1], out[2]


def solution(mesh):
    in_specs = (
        P("seq", "head"), P(None, "head"), P(None, "head"), P(None, "head"),
        P("seq", "head"), P("seq", "head"), P(),
    )
    out_specs = (P("seq", "head"),) * 3
    return jax.shard_map(local, mesh=mesh, in_specs=in_specs, out_specs=out_specs, check_vma=False)
```

```python
import jax
import jax.numpy as jnp
from jax import lax
from jax.experimental import pallas as pl
from jax.experimental.pallas import tpu as pltpu
from jax.sharding import PartitionSpec as P

HEAD = 128
SCALE = HEAD ** (-0.5)
MESH = pl.DeviceIdType.MESH
BF16, F32 = jnp.bfloat16, jnp.float32
AROUND = (1, 3, 2)


def dot(a, b, da, db):
    return lax.dot_general(a, b, (((da,), (db,)), ((), ())), preferred_element_type=F32)


def kernel(
    tok, wq, wk, wv, up, ldt_in, segv_in, segs_in,
    out,
    ldt, segv, segs, x_all, w_all, qkv, qkv_x, upb, up_x, ct,
    gl, inm, outm, carry, lst, rst, inc, ret, grad, rows_x, rows_r,
    x_first, x_rest, c_first, c_rest, z_recv, u_recv, g_mate, g_recv, d_recv, o_recv, sends, loc, alive,
):
    seq, head = lax.axis_index("seq"), lax.axis_index("head")
    z, c = seq // 2, seq % 2
    x, y = head // 4, head % 4
    other = 1 - c
    zs = [(z + i) % 8 for i in range(8)]

    def plane_at(dx, dy):
        return ((x + dx) % 4) * 4 + (y + dy) % 4

    def at(dz=0, dx=0, dy=0, core=None):
        return {"seq": zs[dz] * 2 + (c if core is None else core), "head": plane_at(dx, dy)}

    partner = at(core=other)
    barrier = pltpu.get_barrier_semaphore()
    near = [partner] + [at(dx=i) for i in AROUND] + [at(dy=i) for i in AROUND] + [at(dz=i, core=j) for i in (1, 7) for j in (c, other)]
    for dev in near:
        pl.semaphore_signal(barrier, inc=1, device_id=dev, device_id_type=MESH)

    def fetch(src, dst, i):
        copy = pltpu.make_async_copy(src, dst, loc.at[i])
        copy.start()
        return copy

    def lanes(i):
        return pl.ds(pl.multiple_of(i * 128, 128), 128)

    own_tok = fetch(tok, x_all.at[head], 0)
    own_ldt = fetch(ldt_in, ldt, 2)
    own_up = fetch(up.at[:, lanes(c)], upb.at[seq, 0:128], 3)
    oth_up = fetch(up.at[:, lanes(other)], up_x.at[0:128], 4)
    seg_v = fetch(segv_in, segv, 5)
    seg_s = fetch(segs_in, segs, 6)
    weights = [fetch(w, w_all.at[i], 7 + i) for i, w in enumerate((wq, wk, wv))]

    own_tok.wait()
    pl.semaphore_wait(barrier, len(near))

    sent = {}

    def send(kind, src, dst, recv, dev):
        rows = src.dtype.itemsize
        for n in src.shape:
            rows *= n
        sent[kind] = sent.get(kind, 0) + rows // 512
        pltpu.make_async_remote_copy(
            src_ref=src, dst_ref=dst, send_sem=sends.at[kind], recv_sem=recv, device_id=dev, device_id_type=MESH
        ).start()

    def described(view, recv):
        return pltpu.make_async_remote_copy(
            src_ref=view, dst_ref=view, send_sem=sends.at[0], recv_sem=recv, device_id=partner, device_id_type=MESH
        )

    def arrived(view, recv):
        described(view, recv).wait_recv()

    def arrived_rows(rows, recv):
        arrived(w_all.at[0, 0:rows], recv)

    def plane(kind, unit, rows, first, rest):
        def there(half, stage, d):
            return at(dx=d) if half == stage else at(dy=d)

        def own():
            for half in (0, 1):
                for j, d in enumerate(AROUND):
                    view = unit(head, half)
                    send(kind, view, view, first.at[half, j], there(half, 0, d))
            for half in (0, 1):
                for d in AROUND:
                    view = unit(head, half)
                    send(kind, view, view, rest, there(half, 1, d))

        def middle():
            for j, d in enumerate(AROUND):
                for half in (0, 1):
                    view = unit(plane_at(-d, 0) if half == 0 else plane_at(0, -d), half)
                    arrived(view, first.at[half, j])
                    for e in AROUND:
                        send(kind, view, view, rest, there(half, 1, e))

        def end():
            arrived_rows(24 * rows, rest)

        return own, middle, end

    def x_unit(k):
        return lambda h, half: x_all.at[h, 64 * half + 32 * k : 64 * half + 32 * (k + 1)]

    def c_unit(h, half):
        return ct.at[h // 8, 4 * half : 4 * (half + 1), c, h % 8]

    def up_own():
        send(2, up_x, upb.at[seq], u_recv.at[8], partner)
        for i, j in ((1, 0), (7, 4)):
            send(2, upb.at[seq], upb.at[seq], u_recv.at[j], at(dz=i))
            send(2, up_x, upb.at[seq], u_recv.at[j], at(dz=i, core=other))

    def up_hop(d):
        below, above = zs[8 - d] * 2, zs[d] * 2
        count = 2 if d < 4 else 1
        arrived(upb.at[0:count], u_recv.at[d - 1])
        if d < 4:
            for parity in (c, other) if d < 3 else (c,):
                send(2, upb.at[below + parity], upb.at[below + parity], u_recv.at[d], at(dz=1))
        arrived(upb.at[0:count], u_recv.at[4 + d - 1])
        if d < 4:
            for parity in (c, other) if d < 3 else (other,):
                send(2, upb.at[above + parity], upb.at[above + parity], u_recv.at[4 + d], at(dz=7))

    def g_to_next(s, p, i, d, both=True, down=False):
        view = qkv.at[s, i]
        if both or not down:
            send(3, view, view, g_recv.at[((0 * 4 + d) * 2 + p) * 3 + i], at(dz=1))
        if both or down:
            send(3, view, view, g_recv.at[((1 * 4 + d) * 2 + p) * 3 + i], at(dz=7))

    def g_own():
        for i in range(3):
            g_to_next(seq, 0, i, 0)
        for i in range(3):
            send(3, qkv_x.at[i], qkv.at[seq, i], g_mate.at[i], partner)
            for j, dz in ((0, 1), (1, 7)):
                send(3, qkv_x.at[i], qkv.at[seq, i], g_recv.at[(j * 4 * 2 + 1) * 3 + i], at(dz=dz, core=other))

    def g_from_mate():
        for i in range(3):
            arrived(qkv.at[z * 2 + other, i], g_mate.at[i])
        arrived(upb.at[z * 2 + other], u_recv.at[8])

    def g_hop(d, p):
        parity = c if p == 0 else other
        for i in range(3):
            if d < 4 or p == 0:
                s = zs[8 - d] * 2 + parity
                arrived(qkv.at[s, i], g_recv.at[((0 * 4 + d - 1) * 2 + p) * 3 + i])
                if d < 3 or (d == 3 and p == 0):
                    g_to_next(s, p, i, d, both=False)
            if d < 4 or p == 1:
                s = zs[d] * 2 + parity
                arrived(qkv.at[s, i], g_recv.at[((1 * 4 + d - 1) * 2 + p) * 3 + i])
                if d < 3 or (d == 3 and p == 1):
                    g_to_next(s, p, i, d, both=False, down=True)

    def project():
        for i in range(3):
            acc = dot(x_all[0], w_all[i, 0:256, :], 1, 0)
            for h in range(1, 16):
                acc = acc + dot(x_all[h], w_all[i, 256 * h : 256 * (h + 1), :], 1, 0)
            acc = acc.astype(BF16)
            qkv[seq, i] = jnp.where(c == 0, acc[:, :128], acc[:, 128:])
            qkv_x[i] = jnp.where(c == 0, acc[:, 128:], acc[:, :128])

    a_own, a_mid, a_end = zip(*[plane(0, x_unit(k), 32, x_first.at[k], x_rest.at[k]) for k in (0, 1)])
    c_own, c_mid, c_end = plane(1, c_unit, 64, c_first, c_rest)

    a_own[0]()
    a_own[1]()

    own_ldt.wait()
    total = jnp.concatenate([ldt[...], jnp.zeros((6, 128), F32)], axis=0)
    lane = lax.broadcasted_iota(jnp.int32, (8, 128), 1)
    for k in (1, 2, 4, 8, 16, 32, 64):
        total = total + jnp.where(lane >= k, pltpu.roll(total, k, 1), 0.0)

    def in_parts(row):
        hi = row.astype(BF16)
        rest = row - hi.astype(F32)
        mid = rest.astype(BF16)
        low = (rest - mid.astype(F32)).astype(BF16)
        return jnp.concatenate([hi.astype(F32), mid.astype(F32), low.astype(F32), jnp.zeros((5, 128), F32)], axis=0).astype(BF16)

    lo, hi = in_parts(total[0:1]), in_parts(total[1:2])
    upb[seq, 128:136] = jnp.where(c == 0, lo, hi)
    up_x[128:136] = jnp.where(c == 0, hi, lo)

    own_up.wait()
    oth_up.wait()
    up_own()
    a_mid[0]()
    a_mid[1]()
    up_hop(1)
    for i in (2, 6):
        pl.semaphore_signal(alive, inc=1, device_id=at(dz=i), device_id_type=MESH)
    for copy in weights:
        copy.wait()
    seg_v.wait()
    seg_s.wait()
    a_end[0]()
    up_hop(2)
    a_end[1]()

    f, group = head // 8, head % 8

    def slice_of(zt):
        return x_all.at[2 * zt + f, pl.ds(pl.multiple_of(group * 16, 16), 16)]

    own_slice = fetch(slice_of(z), ct.at[f, z, c, group], 0)
    pl.semaphore_wait(alive, 2)
    for i in (4, 3, 5, 2, 6, 1, 7):
        send(4, slice_of(zs[i]), ct.at[f, z, c, group], z_recv.at[0], at(dz=i))
    project()
    g_own()
    g_from_mate()

    ti = lax.broadcasted_iota(jnp.int32, (128, 128), 0)
    si = lax.broadcasted_iota(jnp.int32, (128, 128), 1)

    def part(b, i):
        return qkv[b, i]

    def attend(blocks):
        done = []
        for b in blocks:
            q, k, v, u = part(b, 0), part(b, 1), part(b, 2), upb[b, 0:128]
            parts = upb[b, 128:136].astype(F32)
            row = parts[0:1] + parts[1:2] + parts[2:3]
            before = segs[jnp.maximum(b * 128 - 1, 0)]
            previous = jnp.where(b > 0, before, -1).astype(F32)
            last = segs[b * 128 + 127].astype(F32)
            ls_s = jnp.broadcast_to(row, (128, 128))
            ls_t = ls_s.T
            seg_s = jnp.broadcast_to(segv[pl.ds(b, 1), :], (128, 128)).astype(F32)
            seg_t = seg_s.T
            same = (seg_s == seg_t) & (ti >= si)
            decay = jnp.where(same, SCALE * jnp.exp(jnp.where(same, ls_t - ls_s, 0.0)), 0.0)
            ls_last = row[:, 127:128]
            inflow = jnp.where(seg_t == previous, jnp.exp(ls_t), 0.0)
            outflow = jnp.where(seg_t == last, jnp.exp(ls_last - ls_t), 0.0)
            keep = jnp.where(last == previous, jnp.exp(ls_last), 0.0)
            a_qk = (decay * dot(q, k, 1, 1)).astype(BF16)
            a_up = (decay * dot(u, v, 1, 1)).astype(BF16)
            wk_ = (SCALE * outflow * k.astype(F32)).astype(BF16)
            wq_ = (SCALE * inflow * q.astype(F32)).astype(BF16)
            done.append((
                inflow, outflow, jnp.broadcast_to(keep, (8, 128)), dot(a_up, k, 1, 0), dot(a_up, q, 0, 0),
                dot(a_qk, u, 0, 0), dot(wk_, v, 0, 0), dot(wq_, u, 0, 0),
            ))
        for b, (inflow, outflow, keep, gq, gk, gv, ls, rs) in zip(blocks, done):
            inm[b], outm[b], carry[b] = inflow, outflow, keep
            gl[b, 0], gl[b, 1], gl[b, 2] = gq, gk, gv
            lst[b], rst[b] = ls, rs

    def c_begin():
        own_slice.wait()
        arrived_rows(7 * 16, z_recv.at[0])
        c_own()

    def c_share():
        c_end()
        for i in (0, 1):
            view = ct.at[i, :, c]
            send(5, view, view, d_recv.at[i], partner)

    attend((seq, z * 2 + other))
    side = {(1, 0): c_begin, (2, 0): c_mid, (3, 1): c_share}
    for d in (1, 2, 3):
        for p in (0, 1):
            parity = c if p == 0 else other
            g_hop(d, p)
            attend((zs[8 - d] * 2 + parity, zs[d] * 2 + parity))
            if (d, p) == (1, 1):
                up_hop(3)
            if (d, p) == (3, 0):
                up_hop(4)
            if (d, p) in side:
                side[d, p]()
    for p in (0, 1):
        g_hop(4, p)
    attend((zs[4] * 2, zs[4] * 2 + 1))

    def forward(b, state):
        inc[b] = state.astype(BF16)
        return carry[b][0:1] * state + lst[b]

    lax.fori_loop(0, 16, forward, jnp.zeros((128, 128), F32))

    def backward(i, state):
        b = 15 - i
        ret[b] = state.astype(BF16)
        return carry[b][0:1] * state + rst[b]

    lax.fori_loop(0, 16, backward, jnp.zeros((128, 128), F32))

    def finish(i, carry_):
        done = []
        for b in (4 * i, 4 * i + 1, 4 * i + 2, 4 * i + 3):
            inflow, outflow = inm[b], outm[b]
            done.append((
                gl[b, 0] + inflow * dot(upb[b, 0:128], inc[b], 1, 1),
                gl[b, 1] + outflow * dot(part(b, 2), ret[b], 1, 1),
                gl[b, 2] + outflow * dot(part(b, 1), ret[b], 1, 0),
            ))
        for j, parts in enumerate(done):
            for k, value in enumerate(parts):
                grad[4 * i + j, :, 128 * k : 128 * (k + 1)] = value.astype(BF16)
        return carry_

    lax.fori_loop(0, 4, finish, 0)
    for i in (0, 1):
        arrived(ct.at[i, :, other], d_recv.at[i])

    def rows_of(core):
        return dot(ct[core].reshape(2048, 256), grad[...].reshape(2048, 384), 0, 0).astype(BF16)

    rows_x[...] = rows_of(other)
    send(6, rows_x, rows_r, o_recv.at[0], partner)
    mine = rows_of(c)
    for i in range(3):
        out[i, :, lanes(c)] = mine[:, 128 * i : 128 * (i + 1)]
    arrived(rows_r, o_recv.at[0])
    for i in range(3):
        out[i, :, lanes(other)] = rows_r[:, 128 * i : 128 * (i + 1)]
    for kind, rows in sent.items():
        view = upb.at[0:15] if kind == 2 else w_all.at[0, 0:rows]
        pltpu.make_async_remote_copy(
            src_ref=view, dst_ref=view, send_sem=sends.at[kind], recv_sem=loc.at[0], device_id=partner, device_id_type=MESH
        ).wait_send()


def local(tokens, w_query, w_key, w_value, upstream, log_decay, segment):
    hbm = pl.BlockSpec(memory_space=pltpu.HBM)
    dma = pltpu.SemaphoreType.DMA
    out = pl.pallas_call(
        kernel,
        out_shape=jax.ShapeDtypeStruct((3, 256, 256), BF16),
        in_specs=[hbm] * 8,
        out_specs=pl.BlockSpec(memory_space=pltpu.VMEM),
        scratch_shapes=[
            pltpu.VMEM((2, 128), F32),
            pltpu.VMEM((16, 128), jnp.int32),
            pltpu.SMEM((2048,), jnp.int32),
            pltpu.VMEM((16, 128, 256), BF16),
            pltpu.VMEM((3, 4096, 256), BF16),
            pltpu.VMEM((16, 3, 128, 128), BF16),
            pltpu.VMEM((3, 128, 128), BF16),
            pltpu.VMEM((16, 136, 128), BF16),
            pltpu.VMEM((136, 128), BF16),
            pltpu.VMEM((2, 8, 2, 8, 16, 256), BF16),
            pltpu.VMEM((16, 3, 128, 128), F32),
            pltpu.VMEM((16, 128, 128), F32),
            pltpu.VMEM((16, 128, 128), F32),
            pltpu.VMEM((16, 8, 128), F32),
            pltpu.VMEM((16, 128, 128), F32),
            pltpu.VMEM((16, 128, 128), F32),
            pltpu.VMEM((16, 128, 128), BF16),
            pltpu.VMEM((16, 128, 128), BF16),
            pltpu.VMEM((16, 128, 384), BF16),
            pltpu.VMEM((256, 384), BF16),
            pltpu.VMEM((256, 384), BF16),
            dma((2, 2, 3)), dma((2,)),
            dma((2, 3)), dma(()),
            dma((1,)), dma((9,)),
            dma((3,)), dma((48,)),
            dma((2,)), dma((1,)),
            dma((7,)), dma((10,)),
            pltpu.SemaphoreType.REGULAR,
        ],
        compiler_params=pltpu.CompilerParams(
            collective_id=0, has_side_effects=True, vmem_limit_bytes=60 * 1024 * 1024
        ),
    )(
        tokens, w_query, w_key, w_value, upstream,
        log_decay.T, segment.reshape(16, 128), segment,
    )
    return out[0], out[1], out[2]


def solution(mesh):
    in_specs = (
        P("seq", "head"), P(None, "head"), P(None, "head"), P(None, "head"),
        P("seq", "head"), P("seq", "head"), P(),
    )
    out_specs = (P("seq", "head"),) * 3
    return jax.shard_map(local, mesh=mesh, in_specs=in_specs, out_specs=out_specs, check_vma=False)
```

```python
import jax
import jax.numpy as jnp
from jax import lax
from jax.experimental import pallas as pl
from jax.experimental.pallas import tpu as pltpu
from jax.sharding import PartitionSpec as P

HEAD = 128
SCALE = HEAD ** (-0.5)
MESH = pl.DeviceIdType.MESH
BF16, F32 = jnp.bfloat16, jnp.float32
AROUND = (1, 3, 2)


def dot(a, b, da, db):
    return lax.dot_general(a, b, (((da,), (db,)), ((), ())), preferred_element_type=F32)


def kernel(
    tok, wq, wk, wv, up, ldt_in, segv_in, segs_in,
    out,
    ldt, segv, segs, x_all, w_all, qkv, qkv_x, upb, up_x, ct,
    gl, inm, outm, carry, dec, lst, rst, inc, ret, grad, rows_x, rows_r,
    x_first, x_rest, c_first, c_rest, z_recv, u_recv, g_mate, g_recv, d_recv, o_recv, sends, loc, alive,
):
    seq, head = lax.axis_index("seq"), lax.axis_index("head")
    z, c = seq // 2, seq % 2
    x, y = head // 4, head % 4
    other = 1 - c
    zs = [(z + i) % 8 for i in range(8)]

    def plane_at(dx, dy):
        return ((x + dx) % 4) * 4 + (y + dy) % 4

    def at(dz=0, dx=0, dy=0, core=None):
        return {"seq": zs[dz] * 2 + (c if core is None else core), "head": plane_at(dx, dy)}

    partner = at(core=other)
    barrier = pltpu.get_barrier_semaphore()
    near = [partner] + [at(dx=i) for i in AROUND] + [at(dy=i) for i in AROUND] + [at(dz=i, core=j) for i in (1, 7) for j in (c, other)]
    for dev in near:
        pl.semaphore_signal(barrier, inc=1, device_id=dev, device_id_type=MESH)

    def fetch(src, dst, i):
        copy = pltpu.make_async_copy(src, dst, loc.at[i])
        copy.start()
        return copy

    def lanes(i):
        return pl.ds(pl.multiple_of(i * 128, 128), 128)

    own_tok = fetch(tok, x_all.at[head], 0)
    own_ldt = fetch(ldt_in, ldt, 2)
    own_up = fetch(up.at[:, lanes(c)], upb.at[seq, 0:128], 3)
    oth_up = fetch(up.at[:, lanes(other)], up_x.at[0:128], 4)
    seg_v = fetch(segv_in, segv, 5)
    seg_s = fetch(segs_in, segs, 6)
    weights = [fetch(w, w_all.at[i], 7 + i) for i, w in enumerate((wq, wk, wv))]

    own_tok.wait()
    pl.semaphore_wait(barrier, len(near))

    sent = {}

    def send(kind, src, dst, recv, dev):
        rows = src.dtype.itemsize
        for n in src.shape:
            rows *= n
        sent[kind] = sent.get(kind, 0) + rows // 512
        pltpu.make_async_remote_copy(
            src_ref=src, dst_ref=dst, send_sem=sends.at[kind], recv_sem=recv, device_id=dev, device_id_type=MESH
        ).start()

    def described(view, recv):
        return pltpu.make_async_remote_copy(
            src_ref=view, dst_ref=view, send_sem=sends.at[0], recv_sem=recv, device_id=partner, device_id_type=MESH
        )

    def arrived(view, recv):
        described(view, recv).wait_recv()

    def arrived_rows(rows, recv):
        arrived(w_all.at[0, 0:rows], recv)

    def plane(kind, unit, rows, first, rest):
        def there(half, stage, d):
            return at(dx=d) if half == stage else at(dy=d)

        def own():
            for half in (0, 1):
                for j, d in enumerate(AROUND):
                    view = unit(head, half)
                    send(kind, view, view, first.at[half, j], there(half, 0, d))
            for half in (0, 1):
                for d in AROUND:
                    view = unit(head, half)
                    send(kind, view, view, rest, there(half, 1, d))

        def middle():
            for j, d in enumerate(AROUND):
                for half in (0, 1):
                    view = unit(plane_at(-d, 0) if half == 0 else plane_at(0, -d), half)
                    arrived(view, first.at[half, j])
                    for e in AROUND:
                        send(kind, view, view, rest, there(half, 1, e))

        def end():
            arrived_rows(24 * rows, rest)

        return own, middle, end

    def x_unit(k):
        return lambda h, half: x_all.at[h, 64 * half + 32 * k : 64 * half + 32 * (k + 1)]

    def c_unit(h, half):
        return ct.at[h // 8, 4 * half : 4 * (half + 1), c, h % 8]

    def up_own():
        send(2, up_x, upb.at[seq], u_recv.at[8], partner)
        for i, j in ((1, 0), (7, 4)):
            send(2, upb.at[seq], upb.at[seq], u_recv.at[j], at(dz=i))
            send(2, up_x, upb.at[seq], u_recv.at[j], at(dz=i, core=other))

    def up_hop(d):
        below, above = zs[8 - d] * 2, zs[d] * 2
        count = 2 if d < 4 else 1
        arrived(upb.at[0:count], u_recv.at[d - 1])
        if d < 4:
            for parity in (c, other) if d < 3 else (c,):
                send(2, upb.at[below + parity], upb.at[below + parity], u_recv.at[d], at(dz=1))
        arrived(upb.at[0:count], u_recv.at[4 + d - 1])
        if d < 4:
            for parity in (c, other) if d < 3 else (other,):
                send(2, upb.at[above + parity], upb.at[above + parity], u_recv.at[4 + d], at(dz=7))

    def g_to_next(s, p, i, d, both=True, down=False):
        view = qkv.at[s, i]
        if both or not down:
            send(3, view, view, g_recv.at[((0 * 4 + d) * 2 + p) * 3 + i], at(dz=1))
        if both or down:
            send(3, view, view, g_recv.at[((1 * 4 + d) * 2 + p) * 3 + i], at(dz=7))

    def g_own():
        for i in range(3):
            g_to_next(seq, 0, i, 0, both=False)
            send(3, qkv_x.at[i], qkv.at[seq, i], g_recv.at[(1 * 4 * 2 + 1) * 3 + i], at(dz=7, core=other))
        for i in range(3):
            send(3, qkv_x.at[i], qkv.at[seq, i], g_mate.at[i], partner)
        for i in range(3):
            send(3, qkv_x.at[i], qkv.at[seq, i], g_recv.at[1 * 3 + i], at(dz=1, core=other))
            g_to_next(seq, 0, i, 0, both=False, down=True)

    def g_from_mate():
        for i in range(3):
            arrived(qkv.at[z * 2 + other, i], g_mate.at[i])
        arrived(upb.at[z * 2 + other], u_recv.at[8])

    def below(d, p):
        return zs[8 - d] * 2 + (c if p == 0 else other)

    def above(d, p):
        return zs[d] * 2 + (other if p == 0 else c)

    def g_hop(d, p):
        for i in range(3):
            s = below(d, p)
            arrived(qkv.at[s, i], g_recv.at[((0 * 4 + d - 1) * 2 + p) * 3 + i])
            if d < 3 or (d == 3 and p == 0):
                g_to_next(s, p, i, d, both=False)
            s = above(d, p)
            arrived(qkv.at[s, i], g_recv.at[((1 * 4 + d - 1) * 2 + 1 - p) * 3 + i])
            if d < 3 or (d == 3 and p == 0):
                g_to_next(s, 1 - p, i, d, both=False, down=True)

    def project():
        for i in range(3):
            acc = dot(x_all[0], w_all[i, 0:256, :], 1, 0)
            for h in range(1, 16):
                acc = acc + dot(x_all[h], w_all[i, 256 * h : 256 * (h + 1), :], 1, 0)
            acc = acc.astype(BF16)
            qkv[seq, i] = jnp.where(c == 0, acc[:, :128], acc[:, 128:])
            qkv_x[i] = jnp.where(c == 0, acc[:, 128:], acc[:, :128])

    a_own, a_mid, a_end = zip(*[plane(0, x_unit(k), 32, x_first.at[k], x_rest.at[k]) for k in (0, 1)])
    c_own, c_mid, c_end = plane(1, c_unit, 64, c_first, c_rest)

    a_own[0]()

    own_ldt.wait()
    total = jnp.concatenate([ldt[...], jnp.zeros((6, 128), F32)], axis=0)
    lane = lax.broadcasted_iota(jnp.int32, (8, 128), 1)
    for k in (1, 2, 4, 8, 16, 32, 64):
        total = total + jnp.where(lane >= k, pltpu.roll(total, k, 1), 0.0)

    def in_parts(row):
        hi = row.astype(BF16)
        rest = row - hi.astype(F32)
        mid = rest.astype(BF16)
        low = (rest - mid.astype(F32)).astype(BF16)
        return jnp.concatenate([hi.astype(F32), mid.astype(F32), low.astype(F32), jnp.zeros((5, 128), F32)], axis=0).astype(BF16)

    lo, hi = in_parts(total[0:1]), in_parts(total[1:2])
    upb[seq, 128:136] = jnp.where(c == 0, lo, hi)
    up_x[128:136] = jnp.where(c == 0, hi, lo)

    own_up.wait()
    oth_up.wait()
    a_own[1]()
    up_own()
    a_mid[0]()
    a_mid[1]()
    up_hop(1)
    for i in (2, 6):
        pl.semaphore_signal(alive, inc=1, device_id=at(dz=i), device_id_type=MESH)
    for copy in weights:
        copy.wait()
    seg_v.wait()
    seg_s.wait()
    a_end[0]()
    up_hop(2)
    a_end[1]()

    f, group = head // 8, head % 8

    def slice_of(zt):
        return x_all.at[2 * zt + f, pl.ds(pl.multiple_of(group * 16, 16), 16)]

    own_slice = fetch(slice_of(z), ct.at[f, z, c, group], 0)
    pl.semaphore_wait(alive, 2)
    for i in (4, 3, 5, 2, 6, 1, 7):
        send(4, slice_of(zs[i]), ct.at[f, z, c, group], z_recv.at[0], at(dz=i))
    project()
    g_own()
    g_from_mate()

    ti = lax.broadcasted_iota(jnp.int32, (128, 128), 0)
    si = lax.broadcasted_iota(jnp.int32, (128, 128), 1)

    def part(b, i):
        return qkv[b, i]

    def prepared(b):
        parts = upb[b, 128:136].astype(F32)
        row = parts[0:1] + parts[1:2] + parts[2:3]
        before = segs[jnp.maximum(b * 128 - 1, 0)]
        previous = jnp.where(b > 0, before, -1).astype(F32)
        last = segs[b * 128 + 127].astype(F32)
        ls_s = jnp.broadcast_to(row, (128, 128))
        ls_t = ls_s.T
        seg_s = jnp.broadcast_to(segv[pl.ds(b, 1), :], (128, 128)).astype(F32)
        seg_t = seg_s.T
        same = (seg_s == seg_t) & (ti >= si)
        decay = jnp.where(same, SCALE * jnp.exp(jnp.where(same, ls_t - ls_s, 0.0)), 0.0)
        ls_last = row[:, 127:128]
        inflow = jnp.where(seg_t == previous, jnp.exp(ls_t), 0.0)
        outflow = jnp.where(seg_t == last, jnp.exp(ls_last - ls_t), 0.0)
        keep = jnp.where(last == previous, jnp.exp(ls_last), 0.0)
        return decay, inflow, outflow, jnp.broadcast_to(keep, (8, 128))

    def prepare(blocks):
        for j, b in enumerate(blocks):
            dec[j], inm[b], outm[b], carry[b] = prepared(b)

    def attend(blocks, ready=False):
        done = []
        for j, b in enumerate(blocks):
            q, k, v, u = qkv[b, 0], qkv[b, 1], qkv[b, 2], upb[b, 0:128]
            if ready:
                decay, inflow, outflow, keep = dec[j], inm[b], outm[b], None
            else:
                decay, inflow, outflow, keep = prepared(b)
            a_qk = (decay * dot(q, k, 1, 1)).astype(BF16)
            a_up = (decay * dot(u, v, 1, 1)).astype(BF16)
            wk_ = (SCALE * outflow * k.astype(F32)).astype(BF16)
            wq_ = (SCALE * inflow * q.astype(F32)).astype(BF16)
            done.append((
                inflow, outflow, keep, dot(a_up, k, 1, 0), dot(a_up, q, 0, 0),
                dot(a_qk, u, 0, 0), dot(wk_, v, 0, 0), dot(wq_, u, 0, 0),
            ))
        for b, (inflow, outflow, keep, gq, gk, gv, ls, rs) in zip(blocks, done):
            if not ready:
                inm[b], outm[b], carry[b] = inflow, outflow, keep
            gl[b, 0], gl[b, 1], gl[b, 2] = gq, gk, gv
            lst[b], rst[b] = ls, rs

    def c_begin():
        own_slice.wait()
        arrived_rows(7 * 16, z_recv.at[0])
        c_own()

    def c_share():
        c_end()
        for i in (0, 1):
            view = ct.at[i, :, c]
            send(5, view, view, d_recv.at[i], partner)

    def block(j):
        return (z * 2 + 10 + j) % 16

    def forward(j, state):
        b = block(j)
        inc[b] = state.astype(BF16)
        return carry[b][0:1] * state + lst[b]

    def backward(i, state):
        b = block(29 - i)
        ret[b] = state.astype(BF16)
        return carry[b][0:1] * state + rst[b]

    def finish(start, count):
        def run(i, carry_):
            done = []
            for b in [block(start + count * i + j) for j in range(count)]:
                inflow, outflow = inm[b], outm[b]
                done.append((b, (
                    gl[b, 0] + inflow * dot(upb[b, 0:128], inc[b], 1, 1),
                    gl[b, 1] + outflow * dot(qkv[b, 2], ret[b], 1, 1),
                    gl[b, 2] + outflow * dot(qkv[b, 1], ret[b], 1, 0),
                )))
            for b, parts in done:
                for k, value in enumerate(parts):
                    grad[b, :, 128 * k : 128 * (k + 1)] = value.astype(BF16)
            return carry_
        return run

    last = (zs[4] * 2, zs[4] * 2 + 1)
    attend((seq, z * 2 + other))
    c_begin()
    for d in (1, 2, 3):
        for p in (0, 1):
            g_hop(d, p)
            if (d, p) == (2, 0):
                c_mid()
            if (d, p) == (3, 1):
                c_share()
            attend((below(d, p), above(d, p)))
            if (d, p) == (1, 1):
                up_hop(3)
            if (d, p) == (3, 0):
                up_hop(4)
                prepare(last)
    zero = jnp.zeros((128, 128), F32)
    state_in = lax.fori_loop(0, 10, forward, zero)
    state_back = lax.fori_loop(0, 10, backward, zero)
    finish(4, 6)(0, 0)
    g_hop(4, 0)
    attend(last, ready=True)
    lax.fori_loop(10, 20, forward, state_in)
    lax.fori_loop(10, 20, backward, state_back)
    lax.fori_loop(0, 2, finish(10, 5), 0)
    for i in (0, 1):
        arrived(ct.at[i, :, other], d_recv.at[i])

    def rows_of(core):
        return dot(ct[core].reshape(2048, 256), grad[...].reshape(2048, 384), 0, 0).astype(BF16)

    rows_x[...] = rows_of(other)
    send(6, rows_x, rows_r, o_recv.at[0], partner)
    mine = rows_of(c)
    for i in range(3):
        out[i, :, lanes(c)] = mine[:, 128 * i : 128 * (i + 1)]
    arrived(rows_r, o_recv.at[0])
    for i in range(3):
        out[i, :, lanes(other)] = rows_r[:, 128 * i : 128 * (i + 1)]
    for kind, rows in sent.items():
        view = upb.at[0:15] if kind == 2 else w_all.at[0, 0:rows]
        pltpu.make_async_remote_copy(
            src_ref=view, dst_ref=view, send_sem=sends.at[kind], recv_sem=loc.at[0], device_id=partner, device_id_type=MESH
        ).wait_send()


def local(tokens, w_query, w_key, w_value, upstream, log_decay, segment):
    hbm = pl.BlockSpec(memory_space=pltpu.HBM)
    dma = pltpu.SemaphoreType.DMA
    out = pl.pallas_call(
        kernel,
        out_shape=jax.ShapeDtypeStruct((3, 256, 256), BF16),
        in_specs=[hbm] * 8,
        out_specs=pl.BlockSpec(memory_space=pltpu.VMEM),
        scratch_shapes=[
            pltpu.VMEM((2, 128), F32),
            pltpu.VMEM((16, 128), jnp.int32),
            pltpu.SMEM((2048,), jnp.int32),
            pltpu.VMEM((16, 128, 256), BF16),
            pltpu.VMEM((3, 4096, 256), BF16),
            pltpu.VMEM((16, 3, 128, 128), BF16),
            pltpu.VMEM((3, 128, 128), BF16),
            pltpu.VMEM((16, 136, 128), BF16),
            pltpu.VMEM((136, 128), BF16),
            pltpu.VMEM((2, 8, 2, 8, 16, 256), BF16),
            pltpu.VMEM((16, 3, 128, 128), F32),
            pltpu.VMEM((16, 128, 128), F32),
            pltpu.VMEM((16, 128, 128), F32),
            pltpu.VMEM((16, 8, 128), F32),
            pltpu.VMEM((2, 128, 128), F32),
            pltpu.VMEM((16, 128, 128), F32),
            pltpu.VMEM((16, 128, 128), F32),
            pltpu.VMEM((16, 128, 128), BF16),
            pltpu.VMEM((16, 128, 128), BF16),
            pltpu.VMEM((16, 128, 384), BF16),
            pltpu.VMEM((256, 384), BF16),
            pltpu.VMEM((256, 384), BF16),
            dma((2, 2, 3)), dma((2,)),
            dma((2, 3)), dma(()),
            dma((1,)), dma((9,)),
            dma((3,)), dma((48,)),
            dma((2,)), dma((1,)),
            dma((7,)), dma((10,)),
            pltpu.SemaphoreType.REGULAR,
        ],
        compiler_params=pltpu.CompilerParams(
            collective_id=0, has_side_effects=True, vmem_limit_bytes=40 * 1024 * 1024
        ),
    )(*[
        pltpu.with_memory_space_constraint(a, pltpu.HBM)
        for a in (
            tokens, w_query, w_key, w_value, upstream,
            log_decay.T, segment.reshape(16, 128), segment,
        )
    ])
    return out[0], out[1], out[2]


def solution(mesh):
    in_specs = (
        P("seq", "head"), P(None, "head"), P(None, "head"), P(None, "head"),
        P("seq", "head"), P("seq", "head"), P(),
    )
    out_specs = (P("seq", "head"),) * 3
    return jax.shard_map(local, mesh=mesh, in_specs=in_specs, out_specs=out_specs, check_vma=False)
```

```python
import jax
import jax.numpy as jnp
from jax import lax
from jax.experimental import pallas as pl
from jax.experimental.pallas import tpu as pltpu
from jax.sharding import PartitionSpec as P

HEAD = 128
SCALE = HEAD ** (-0.5)
MESH = pl.DeviceIdType.MESH
BF16, F32 = jnp.bfloat16, jnp.float32
AROUND = (1, 3, 2)


def dot(a, b, da, db):
    return lax.dot_general(a, b, (((da,), (db,)), ((), ())), preferred_element_type=F32)


def kernel(
    tok, wq, wk, wv, up, ldt_in, segv_in, segs_in,
    out,
    ldt, segv, segs, x_all, w_all, qkv, qkv_x, upb, up_x, ct,
    gl, inm, outm, carry, dec, lst, rst, inc, ret, grads, rows_a, rows_x, rows_r,
    x_first, x_rest, c_first, c_rest, z_recv, u_recv, g_mate, g_recv, d_recv, o_recv, sends, loc, alive,
):
    seq, head = lax.axis_index("seq"), lax.axis_index("head")
    z, c = seq // 2, seq % 2
    x, y = head // 4, head % 4
    other = 1 - c
    zs = [(z + i) % 8 for i in range(8)]

    def plane_at(dx, dy):
        return ((x + dx) % 4) * 4 + (y + dy) % 4

    def at(dz=0, dx=0, dy=0, core=None):
        return {"seq": zs[dz] * 2 + (c if core is None else core), "head": plane_at(dx, dy)}

    partner = at(core=other)
    barrier = pltpu.get_barrier_semaphore()
    near = [partner] + [at(dx=i) for i in AROUND] + [at(dy=i) for i in AROUND] + [at(dz=i, core=j) for i in (1, 7, 2, 6) for j in (c, other)]
    for dev in near:
        pl.semaphore_signal(barrier, inc=1, device_id=dev, device_id_type=MESH)

    def fetch(src, dst, i):
        copy = pltpu.make_async_copy(src, dst, loc.at[i])
        copy.start()
        return copy

    def lanes(i):
        return pl.ds(pl.multiple_of(i * 128, 128), 128)

    own_tok = fetch(tok, x_all.at[head], 0)
    own_ldt = fetch(ldt_in, ldt, 2)
    own_up = fetch(up.at[:, lanes(c)], upb.at[seq, 0:128], 3)
    oth_up = fetch(up.at[:, lanes(other)], up_x.at[0:128], 4)
    seg_v = fetch(segv_in, segv, 5)
    seg_s = fetch(segs_in, segs, 6)
    weights = [fetch(w, w_all.at[i], 7 + i) for i, w in enumerate((wq, wk, wv))]

    own_tok.wait()
    pl.semaphore_wait(barrier, len(near))
    for i in (1, 7, 2, 6):
        pl.semaphore_signal(alive, inc=1, device_id=at(dz=i), device_id_type=MESH)

    sent = {}

    def send(kind, src, dst, recv, dev):
        rows = src.dtype.itemsize
        for n in src.shape:
            rows *= n
        sent[kind] = sent.get(kind, 0) + rows // 512
        pltpu.make_async_remote_copy(
            src_ref=src, dst_ref=dst, send_sem=sends.at[kind], recv_sem=recv, device_id=dev, device_id_type=MESH
        ).start()

    def described(view, recv):
        return pltpu.make_async_remote_copy(
            src_ref=view, dst_ref=view, send_sem=sends.at[0], recv_sem=recv, device_id=partner, device_id_type=MESH
        )

    def arrived(view, recv):
        described(view, recv).wait_recv()

    def arrived_rows(rows, recv):
        arrived(w_all.at[0, 0:rows], recv)

    def plane(kind, unit, rows, first, rest):
        def there(half, stage, d):
            return at(dx=d) if half == stage else at(dy=d)

        def own():
            for half in (0, 1):
                for j, d in enumerate(AROUND):
                    view = unit(head, half)
                    send(kind, view, view, first.at[half, j], there(half, 0, d))
            for half in (0, 1):
                for d in AROUND:
                    view = unit(head, half)
                    send(kind, view, view, rest, there(half, 1, d))

        def middle():
            for j, d in enumerate(AROUND):
                for half in (0, 1):
                    view = unit(plane_at(-d, 0) if half == 0 else plane_at(0, -d), half)
                    arrived(view, first.at[half, j])
                    for e in AROUND:
                        send(kind, view, view, rest, there(half, 1, e))

        def end():
            arrived_rows(24 * rows, rest)

        return own, middle, end

    def x_unit(k):
        return lambda h, half: x_all.at[h, 64 * k + 32 * half : 64 * k + 32 * (half + 1)]

    def c_unit(h, half):
        return ct.at[h // 8, 4 * half : 4 * (half + 1), c, h % 8]

    def up_own():
        send(2, up_x, upb.at[seq], u_recv.at[8], partner)
        for i, j in ((1, 0), (7, 4), (2, 1), (6, 5)):
            send(2, upb.at[seq], upb.at[seq], u_recv.at[j], at(dz=i))
            send(2, up_x, upb.at[seq], u_recv.at[j], at(dz=i, core=other))

    def up_hop(d):
        below_, above_ = zs[8 - d] * 2, zs[d] * 2
        count = 2 if d < 4 else 1
        arrived(upb.at[0:count], u_recv.at[d - 1])
        if d in (2, 3):
            for parity in (c, other) if d < 3 else (c,):
                send(2, upb.at[below_ + parity], upb.at[below_ + parity], u_recv.at[d], at(dz=1))
        arrived(upb.at[0:count], u_recv.at[4 + d - 1])
        if d in (2, 3):
            for parity in (c, other) if d < 3 else (other,):
                send(2, upb.at[above_ + parity], upb.at[above_ + parity], u_recv.at[4 + d], at(dz=7))

    def g_send(src, s, k, down, d, p, core):
        send(3, src, qkv.at[s, k], g_recv.at[((down * 4 + d) * 2 + p) * 2 + k], at(dz=7 if down else 1, core=core))

    def g_own(k):
        g_send(qkv.at[seq, k], seq, k, 0, 0, 0, c)
        g_send(qkv_x.at[k], seq, k, 1, 0, 1, other)
        send(3, qkv_x.at[k], qkv.at[seq, k], g_mate.at[k], partner)
        g_send(qkv_x.at[k], seq, k, 0, 0, 1, other)
        g_send(qkv.at[seq, k], seq, k, 1, 0, 0, c)

    def g_from_mate():
        for k in (0, 1):
            arrived(qkv.at[z * 2 + other, k], g_mate.at[k])
        arrived(upb.at[z * 2 + other], u_recv.at[8])

    def below(d, p):
        return zs[8 - d] * 2 + (c if p == 0 else other)

    def above(d, p):
        return zs[d] * 2 + (other if p == 0 else c)

    def g_hop(d, p, k):
        for down, s, q in ((0, below(d, p), p), (1, above(d, p), 1 - p)):
            arrived(qkv.at[s, k], g_recv.at[((down * 4 + d - 1) * 2 + q) * 2 + k])
            if d < 3 or (d == 3 and p == 0):
                g_send(qkv.at[s, k], s, k, down, d, q, c)

    def project(k):
        for i in range(3):
            acc = dot(x_all[0, 64 * k : 64 * (k + 1)], w_all[i, 0:256, :], 1, 0)
            for h in range(1, 16):
                acc = acc + dot(x_all[h, 64 * k : 64 * (k + 1)], w_all[i, 256 * h : 256 * (h + 1), :], 1, 0)
            acc = acc.astype(BF16)
            qkv[seq, k, i] = jnp.where(c == 0, acc[:, :128], acc[:, 128:])
            qkv_x[k, i] = jnp.where(c == 0, acc[:, 128:], acc[:, :128])

    a_own, a_mid, a_end = zip(*[plane(0, x_unit(k), 32, x_first.at[k], x_rest.at[k]) for k in (0, 1)])
    c_own, c_mid, c_end = plane(1, c_unit, 64, c_first, c_rest)

    a_own[0]()

    own_ldt.wait()
    total = jnp.concatenate([ldt[...], jnp.zeros((6, 128), F32)], axis=0)
    lane = lax.broadcasted_iota(jnp.int32, (8, 128), 1)
    for k in (1, 2, 4, 8, 16, 32, 64):
        total = total + jnp.where(lane >= k, pltpu.roll(total, k, 1), 0.0)

    def in_parts(row):
        hi = row.astype(BF16)
        rest = row - hi.astype(F32)
        mid = rest.astype(BF16)
        low = (rest - mid.astype(F32)).astype(BF16)
        return jnp.concatenate([hi.astype(F32), mid.astype(F32), low.astype(F32), jnp.zeros((5, 128), F32)], axis=0).astype(BF16)

    lo, hi = in_parts(total[0:1]), in_parts(total[1:2])
    upb[seq, 128:136] = jnp.where(c == 0, lo, hi)
    up_x[128:136] = jnp.where(c == 0, hi, lo)

    own_up.wait()
    oth_up.wait()
    a_own[1]()
    up_own()
    a_mid[0]()
    a_mid[1]()
    up_hop(1)
    up_hop(2)
    for copy in weights:
        copy.wait()
    seg_v.wait()
    seg_s.wait()
    a_end[0]()
    project(0)
    a_end[1]()

    f, group = head // 8, head % 8

    def slice_of(zt):
        return x_all.at[2 * zt + f, pl.ds(pl.multiple_of(group * 16, 16), 16)]

    own_slice = fetch(slice_of(z), ct.at[f, z, c, group], 0)
    pl.semaphore_wait(alive, 4)
    for i in (4, 3, 5, 2, 6, 1, 7):
        send(4, slice_of(zs[i]), ct.at[f, z, c, group], z_recv.at[0], at(dz=i))
    g_own(0)
    project(1)
    g_own(1)
    g_from_mate()

    ti = lax.broadcasted_iota(jnp.int32, (128, 128), 0)
    si = lax.broadcasted_iota(jnp.int32, (128, 128), 1)

    def part(b, i):
        return jnp.concatenate([qkv[b, 0, i], qkv[b, 1, i]], axis=0)

    def prepared(b):
        parts = upb[b, 128:136].astype(F32)
        row = parts[0:1] + parts[1:2] + parts[2:3]
        before = segs[jnp.maximum(b * 128 - 1, 0)]
        previous = jnp.where(b > 0, before, -1).astype(F32)
        last = segs[b * 128 + 127].astype(F32)
        ls_s = jnp.broadcast_to(row, (128, 128))
        ls_t = ls_s.T
        seg_s = jnp.broadcast_to(segv[pl.ds(b, 1), :], (128, 128)).astype(F32)
        seg_t = seg_s.T
        same = (seg_s == seg_t) & (ti >= si)
        decay = jnp.where(same, SCALE * jnp.exp(jnp.where(same, ls_t - ls_s, 0.0)), 0.0)
        ls_last = row[:, 127:128]
        inflow = jnp.where(seg_t == previous, jnp.exp(ls_t), 0.0)
        outflow = jnp.where(seg_t == last, jnp.exp(ls_last - ls_t), 0.0)
        keep = jnp.where(last == previous, jnp.exp(ls_last), 0.0)
        return decay, inflow, outflow, jnp.broadcast_to(keep, (8, 128))

    def prepare(blocks):
        for j, b in enumerate(blocks):
            dec[j], inm[b], outm[b], carry[b] = prepared(b)

    def attend(blocks, ready=False):
        done = []
        for j, b in enumerate(blocks):
            q, k, v, u = part(b, 0), part(b, 1), part(b, 2), upb[b, 0:128]
            if ready:
                decay, inflow, outflow, keep = dec[j], inm[b], outm[b], None
            else:
                decay, inflow, outflow, keep = prepared(b)
            a_qk = (decay * dot(q, k, 1, 1)).astype(BF16)
            a_up = (decay * dot(u, v, 1, 1)).astype(BF16)
            wk_ = (SCALE * outflow * k.astype(F32)).astype(BF16)
            wq_ = (SCALE * inflow * q.astype(F32)).astype(BF16)
            done.append((
                inflow, outflow, keep, dot(a_up, k, 1, 0), dot(a_up, q, 0, 0),
                dot(a_qk, u, 0, 0), dot(wk_, v, 0, 0), dot(wq_, u, 0, 0),
            ))
        for b, (inflow, outflow, keep, gq, gk, gv, ls, rs) in zip(blocks, done):
            if not ready:
                inm[b], outm[b], carry[b] = inflow, outflow, keep
            gl[b, 0], gl[b, 1], gl[b, 2] = gq, gk, gv
            lst[b], rst[b] = ls, rs

    def c_begin():
        own_slice.wait()
        arrived_rows(7 * 16, z_recv.at[0])
        c_own()

    def c_share():
        c_end()
        for i in (0, 1):
            view = ct.at[i, :, c]
            send(5, view, view, d_recv.at[i], partner)

    def block(j):
        return (z * 2 + 10 + j) % 16

    def forward(j, state):
        b = block(j)
        inc[b] = state.astype(BF16)
        return carry[b][0:1] * state + lst[b]

    def backward(i, state):
        b = block(29 - i)
        ret[b] = state.astype(BF16)
        return carry[b][0:1] * state + rst[b]

    def finish(start, count):
        def run(i, carry_):
            done = []
            for b in [block(start + count * i + j) for j in range(count)]:
                inflow, outflow = inm[b], outm[b]
                done.append((b, (
                    gl[b, 0] + inflow * dot(upb[b, 0:128], inc[b], 1, 1),
                    gl[b, 1] + outflow * dot(part(b, 2), ret[b], 1, 1),
                    gl[b, 2] + outflow * dot(part(b, 1), ret[b], 1, 0),
                )))
            for b, parts in done:
                for k, value in enumerate(parts):
                    grads[b // 2, b % 2, :, 128 * k : 128 * (k + 1)] = value.astype(BF16)
            return carry_
        return run

    last = (zs[4] * 2, zs[4] * 2 + 1)
    attend((seq, z * 2 + other))
    up_hop(3)
    for d in (1, 2, 3):
        g_hop(d, 0, 0)
        g_hop(d, 1, 0)
        if d == 1:
            c_begin()
        g_hop(d, 0, 1)
        if d == 2:
            c_mid()
        attend((below(d, 0), above(d, 0)))
        if d == 3:
            up_hop(4)
            prepare(last)
        g_hop(d, 1, 1)
        attend((below(d, 1), above(d, 1)))
    zero = jnp.zeros((128, 128), F32)
    state_in = lax.fori_loop(0, 10, forward, zero)
    state_back = lax.fori_loop(0, 10, backward, zero)
    finish(4, 6)(0, 0)
    c_share()
    g_hop(4, 0, 0)
    g_hop(4, 0, 1)
    attend(last, ready=True)
    lax.fori_loop(10, 20, forward, state_in)
    lax.fori_loop(10, 20, backward, state_back)
    lax.fori_loop(0, 2, finish(10, 5), 0)
    def rows_of(core, parity):
        right = grads[:, parity].reshape(1024, 384)
        return dot(ct[core, :, parity].reshape(1024, 256), right, 0, 0)

    rows_a[...] = rows_of(other, c)
    for i in (0, 1):
        arrived(ct.at[i, :, other], d_recv.at[i])
    rows_x[...] = (rows_a[...] + rows_of(other, other)).astype(BF16)
    send(6, rows_x, rows_r, o_recv.at[0], partner)
    mine = (rows_of(c, c) + rows_of(c, other)).astype(BF16)
    for i in range(3):
        out[i, :, lanes(c)] = mine[:, 128 * i : 128 * (i + 1)]
    arrived(rows_r, o_recv.at[0])
    for i in range(3):
        out[i, :, lanes(other)] = rows_r[:, 128 * i : 128 * (i + 1)]
    for kind, rows in sent.items():
        view = upb.at[0:15] if kind == 2 else w_all.at[0, 0:rows]
        pltpu.make_async_remote_copy(
            src_ref=view, dst_ref=view, send_sem=sends.at[kind], recv_sem=loc.at[0], device_id=partner, device_id_type=MESH
        ).wait_send()


def local(tokens, w_query, w_key, w_value, upstream, log_decay, segment):
    hbm = pl.BlockSpec(memory_space=pltpu.HBM)
    dma = pltpu.SemaphoreType.DMA
    out = pl.pallas_call(
        kernel,
        out_shape=jax.ShapeDtypeStruct((3, 256, 256), BF16),
        in_specs=[hbm] * 8,
        out_specs=pl.BlockSpec(memory_space=pltpu.VMEM),
        scratch_shapes=[
            pltpu.VMEM((2, 128), F32),
            pltpu.VMEM((16, 128), jnp.int32),
            pltpu.SMEM((2048,), jnp.int32),
            pltpu.VMEM((16, 128, 256), BF16),
            pltpu.VMEM((3, 4096, 256), BF16),
            pltpu.VMEM((16, 2, 3, 64, 128), BF16),
            pltpu.VMEM((2, 3, 64, 128), BF16),
            pltpu.VMEM((16, 136, 128), BF16),
            pltpu.VMEM((136, 128), BF16),
            pltpu.VMEM((2, 8, 2, 8, 16, 256), BF16),
            pltpu.VMEM((16, 3, 128, 128), F32),
            pltpu.VMEM((16, 128, 128), F32),
            pltpu.VMEM((16, 128, 128), F32),
            pltpu.VMEM((16, 8, 128), F32),
            pltpu.VMEM((2, 128, 128), F32),
            pltpu.VMEM((16, 128, 128), F32),
            pltpu.VMEM((16, 128, 128), F32),
            pltpu.VMEM((16, 128, 128), BF16),
            pltpu.VMEM((16, 128, 128), BF16),
            pltpu.VMEM((8, 2, 128, 384), BF16),
            pltpu.VMEM((256, 384), F32),
            pltpu.VMEM((256, 384), BF16),
            pltpu.VMEM((256, 384), BF16),
            dma((2, 2, 3)), dma((2,)),
            dma((2, 3)), dma(()),
            dma((1,)), dma((9,)),
            dma((2,)), dma((32,)),
            dma((2,)), dma((1,)),
            dma((7,)), dma((10,)),
            pltpu.SemaphoreType.REGULAR,
        ],
        compiler_params=pltpu.CompilerParams(
            collective_id=0, has_side_effects=True, vmem_limit_bytes=40 * 1024 * 1024
        ),
    )(*[
        pltpu.with_memory_space_constraint(a, pltpu.HBM)
        for a in (
            tokens, w_query, w_key, w_value, upstream,
            log_decay.T, segment.reshape(16, 128), segment,
        )
    ])
    return out[0], out[1], out[2]


def solution(mesh):
    in_specs = (
        P("seq", "head"), P(None, "head"), P(None, "head"), P(None, "head"),
        P("seq", "head"), P("seq", "head"), P(),
    )
    out_specs = (P("seq", "head"),) * 3
    return jax.shard_map(local, mesh=mesh, in_specs=in_specs, out_specs=out_specs, check_vma=False)
```

```python
import jax
import jax.numpy as jnp
from jax import lax
from jax.experimental import pallas as pl
from jax.experimental.pallas import tpu as pltpu
from jax.sharding import PartitionSpec as P

HEAD = 128
SCALE = HEAD ** (-0.5)
MESH = pl.DeviceIdType.MESH
BF16, F32 = jnp.bfloat16, jnp.float32
AROUND = (1, 3, 2)


def dot(a, b, da, db):
    return lax.dot_general(a, b, (((da,), (db,)), ((), ())), preferred_element_type=F32)


def kernel(
    tok, wq, wk, wv, up, ldt_in, segv_in, segs_in,
    out,
    ldt, segv, segs, x_all, w_all, qkv, qkv_x, upb, up_x, ct,
    gl, inm, outm, carry, dec, lst, rst, inc, ret, grads, rows_a, rows_x, rows_r,
    x_first, x_rest, c_first, c_rest, z_recv, u_recv, g_mate, g_recv, d_recv, o_recv, sends, loc, alive,
):
    seq, head = lax.axis_index("seq"), lax.axis_index("head")
    z, c = seq // 2, seq % 2
    x, y = head // 4, head % 4
    other = 1 - c
    zs = [(z + i) % 8 for i in range(8)]

    def plane_at(dx, dy):
        return ((x + dx) % 4) * 4 + (y + dy) % 4

    def at(dz=0, dx=0, dy=0, core=None):
        return {"seq": zs[dz] * 2 + (c if core is None else core), "head": plane_at(dx, dy)}

    partner = at(core=other)
    barrier = pltpu.get_barrier_semaphore()
    near = [partner] + [at(dx=i) for i in AROUND] + [at(dy=i) for i in AROUND] + [at(dz=i, core=j) for i in (1, 7) for j in (c, other)]
    for dev in near:
        pl.semaphore_signal(barrier, inc=1, device_id=dev, device_id_type=MESH)

    def fetch(src, dst, i):
        copy = pltpu.make_async_copy(src, dst, loc.at[i])
        copy.start()
        return copy

    def lanes(i):
        return pl.ds(pl.multiple_of(i * 128, 128), 128)

    own_tok = fetch(tok, x_all.at[head], 0)
    own_ldt = fetch(ldt_in, ldt, 2)
    own_up = fetch(up.at[:, lanes(c)], upb.at[seq, 0:128], 3)
    oth_up = fetch(up.at[:, lanes(other)], up_x.at[0:128], 4)
    seg_v = fetch(segv_in, segv, 5)
    seg_s = fetch(segs_in, segs, 6)
    for i, w in enumerate((wq, wk, wv)):
        fetch(w, w_all.at[i], 7)

    own_tok.wait()
    pl.semaphore_wait(barrier, len(near))
    for i in (1, 7):
        pl.semaphore_signal(alive.at[0], inc=1, device_id=at(dz=i), device_id_type=MESH)

    sent = {}

    def send(kind, src, dst, recv, dev):
        rows = src.dtype.itemsize
        for n in src.shape:
            rows *= n
        sent[kind] = sent.get(kind, 0) + rows // 512
        pltpu.make_async_remote_copy(
            src_ref=src, dst_ref=dst, send_sem=sends.at[kind], recv_sem=recv, device_id=dev, device_id_type=MESH
        ).start()

    def described(view, recv):
        return pltpu.make_async_remote_copy(
            src_ref=view, dst_ref=view, send_sem=sends.at[0], recv_sem=recv, device_id=partner, device_id_type=MESH
        )

    def arrived(view, recv):
        described(view, recv).wait_recv()

    def arrived_rows(rows, recv):
        arrived(w_all.at[0, 0:rows], recv)

    def plane(kind, unit, rows, first, rest, together=False):
        def there(half, stage, d):
            return at(dx=d) if half == stage else at(dy=d)

        def own():
            for half in (0, 1):
                for j, d in enumerate(AROUND):
                    view = unit(head, half)
                    send(kind, view, view, first.at[0] if together else first.at[half, j], there(half, 0, d))
            for half in (0, 1):
                for d in AROUND:
                    view = unit(head, half)
                    send(kind, view, view, rest, there(half, 1, d))

        def middle():
            if together:
                arrived_rows(6 * rows, first.at[0])
            for j, d in enumerate(AROUND):
                for half in (0, 1):
                    view = unit(plane_at(-d, 0) if half == 0 else plane_at(0, -d), half)
                    if not together:
                        arrived(view, first.at[half, j])
                    for e in AROUND:
                        send(kind, view, view, rest, there(half, 1, e))

        def end():
            arrived_rows(24 * rows, rest)

        return own, middle, end

    def x_unit(k):
        return lambda h, half: x_all.at[h, 64 * k + 32 * half : 64 * k + 32 * (half + 1)]

    def c_unit(h, half):
        return ct.at[h // 4, 4 * half : 4 * (half + 1), c, :, h % 4]

    def up_own():
        send(2, up_x, upb.at[seq], u_recv.at[8], partner)
        for i, j in ((1, 0), (7, 4)):
            send(2, upb.at[seq], upb.at[seq], u_recv.at[j], at(dz=i))
            send(2, up_x, upb.at[seq], u_recv.at[j], at(dz=i, core=other))

    def up_two():
        pl.semaphore_wait(alive.at[0], 2)
        for i in (2, 6):
            pl.semaphore_signal(alive.at[1], inc=1, device_id=at(dz=i), device_id_type=MESH)
        for i, j in ((2, 1), (6, 5)):
            send(2, upb.at[seq], upb.at[seq], u_recv.at[j], at(dz=i))
            send(2, up_x, upb.at[seq], u_recv.at[j], at(dz=i, core=other))

    def up_hop(d):
        below_, above_ = zs[8 - d] * 2, zs[d] * 2
        count = 2 if d < 4 else 1
        arrived(upb.at[0:count], u_recv.at[d - 1])
        if d in (2, 3):
            for parity in (c, other) if d < 3 else (c,):
                send(2, upb.at[below_ + parity], upb.at[below_ + parity], u_recv.at[d], at(dz=1))
        arrived(upb.at[0:count], u_recv.at[4 + d - 1])
        if d in (2, 3):
            for parity in (c, other) if d < 3 else (other,):
                send(2, upb.at[above_ + parity], upb.at[above_ + parity], u_recv.at[4 + d], at(dz=7))

    def g_send(src, s, k, down, d, p, core):
        send(3, src, qkv.at[s, k], g_recv.at[((down * 4 + d) * 2 + p) * 2 + k], at(dz=7 if down else 1, core=core))

    def g_own_first(k):
        g_send(qkv.at[seq, k], seq, k, 0, 0, 0, c)
        g_send(qkv_x.at[k], seq, k, 1, 0, 1, other)
        send(3, qkv_x.at[k], qkv.at[seq, k], g_mate.at[k], partner)

    def g_own_second(k):
        g_send(qkv_x.at[k], seq, k, 0, 0, 1, other)
        g_send(qkv.at[seq, k], seq, k, 1, 0, 0, c)

    def g_from_mate():
        for k in (0, 1):
            arrived(qkv.at[z * 2 + other, k], g_mate.at[k])
        arrived(upb.at[z * 2 + other], u_recv.at[8])

    def below(d, p):
        return zs[8 - d] * 2 + (c if p == 0 else other)

    def above(d, p):
        return zs[d] * 2 + (other if p == 0 else c)

    def g_hop(d, p, k):
        for down, s, q in ((0, below(d, p), p), (1, above(d, p), 1 - p)):
            arrived(qkv.at[s, k], g_recv.at[((down * 4 + d - 1) * 2 + q) * 2 + k])
            if d < 3 or (d == 3 and p == 0):
                g_send(qkv.at[s, k], s, k, down, d, q, c)

    def project(k):
        for i in range(3):
            acc = dot(x_all[0, 64 * k : 64 * (k + 1)], w_all[i, 0:256, :], 1, 0)
            for h in range(1, 16):
                acc = acc + dot(x_all[h, 64 * k : 64 * (k + 1)], w_all[i, 256 * h : 256 * (h + 1), :], 1, 0)
            acc = acc.astype(BF16)
            qkv[seq, k, i] = jnp.where(c == 0, acc[:, :128], acc[:, 128:])
            qkv_x[k, i] = jnp.where(c == 0, acc[:, 128:], acc[:, :128])

    quarter, group = head // 4, head % 4

    def slice_of(zt, k):
        rows = pl.ds(pl.multiple_of(64 * k + 16 * group, 16), 16)
        return x_all.at[2 * zt + quarter // 2, rows, lanes(quarter % 2)]

    own_slices = []

    def slices_out(k):
        own_slices.append(fetch(slice_of(z, k), ct.at[quarter, z, c, k, group], k))
        for i in (4, 3, 5, 2, 6, 1, 7):
            send(3, slice_of(zs[i], k), ct.at[quarter, z, c, k, group], z_recv.at[0], at(dz=i))

    a_own, a_mid, a_end = zip(*[plane(0, x_unit(k), 32, x_first.at[k], x_rest.at[k]) for k in (0, 1)])
    c_own, c_mid, c_end = plane(0, c_unit, 64, c_first, c_rest, together=True)

    a_own[0]()

    own_ldt.wait()
    total = jnp.concatenate([ldt[...], jnp.zeros((6, 128), F32)], axis=0)
    lane = lax.broadcasted_iota(jnp.int32, (8, 128), 1)
    for k in (1, 2, 4, 8, 16, 32, 64):
        total = total + jnp.where(lane >= k, pltpu.roll(total, k, 1), 0.0)

    def in_parts(row):
        hi = row.astype(BF16)
        rest = row - hi.astype(F32)
        mid = rest.astype(BF16)
        low = (rest - mid.astype(F32)).astype(BF16)
        return jnp.concatenate([hi.astype(F32), mid.astype(F32), low.astype(F32), jnp.zeros((5, 128), F32)], axis=0).astype(BF16)

    lo, hi = in_parts(total[0:1]), in_parts(total[1:2])
    upb[seq, 128:136] = jnp.where(c == 0, lo, hi)
    up_x[128:136] = jnp.where(c == 0, hi, lo)

    own_up.wait()
    oth_up.wait()
    a_own[1]()
    up_own()
    up_two()
    a_mid[0]()
    a_mid[1]()
    up_hop(1)
    up_hop(2)
    pltpu.make_async_copy(w_all, w_all, loc.at[7]).wait()
    seg_v.wait()
    seg_s.wait()
    a_end[0]()
    pl.semaphore_wait(alive.at[1], 2)
    slices_out(0)
    project(0)
    a_end[1]()

    slices_out(1)
    g_own_first(0)
    project(1)
    g_own_first(1)
    g_own_second(0)
    g_own_second(1)
    g_from_mate()

    ti = lax.broadcasted_iota(jnp.int32, (128, 128), 0)
    si = lax.broadcasted_iota(jnp.int32, (128, 128), 1)

    def part(b, i):
        return jnp.concatenate([qkv[b, 0, i], qkv[b, 1, i]], axis=0)

    def prepared(b):
        parts = upb[b, 128:136].astype(F32)
        row = parts[0:1] + parts[1:2] + parts[2:3]
        before = segs[jnp.maximum(b * 128 - 1, 0)]
        previous = jnp.where(b > 0, before, -1).astype(F32)
        last = segs[b * 128 + 127].astype(F32)
        ls_s = jnp.broadcast_to(row, (128, 128))
        ls_t = ls_s.T
        seg_s = jnp.broadcast_to(segv[pl.ds(b, 1), :], (128, 128)).astype(F32)
        seg_t = seg_s.T
        same = (seg_s == seg_t) & (ti >= si)
        decay = jnp.where(same, SCALE * jnp.exp(jnp.where(same, ls_t - ls_s, 0.0)), 0.0)
        ls_last = row[:, 127:128]
        inflow = jnp.where(seg_t == previous, jnp.exp(ls_t), 0.0)
        outflow = jnp.where(seg_t == last, jnp.exp(ls_last - ls_t), 0.0)
        keep = jnp.where(last == previous, jnp.exp(ls_last), 0.0)
        return decay, inflow, outflow, jnp.broadcast_to(keep, (8, 128))

    def prepare(blocks):
        for j, b in enumerate(blocks):
            dec[j], inm[b], outm[b], carry[b] = prepared(b)

    def attend(blocks, ready=False):
        done = []
        for j, b in enumerate(blocks):
            q, k, v, u = part(b, 0), part(b, 1), part(b, 2), upb[b, 0:128]
            if ready:
                decay, inflow, outflow, keep = dec[j], inm[b], outm[b], None
            else:
                decay, inflow, outflow, keep = prepared(b)
            a_qk = (decay * dot(q, k, 1, 1)).astype(BF16)
            a_up = (decay * dot(u, v, 1, 1)).astype(BF16)
            wk_ = (SCALE * outflow * k.astype(F32)).astype(BF16)
            wq_ = (SCALE * inflow * q.astype(F32)).astype(BF16)
            done.append((
                inflow, outflow, keep, dot(a_up, k, 1, 0), dot(a_up, q, 0, 0),
                dot(a_qk, u, 0, 0), dot(wk_, v, 0, 0), dot(wq_, u, 0, 0),
            ))
        for b, (inflow, outflow, keep, gq, gk, gv, ls, rs) in zip(blocks, done):
            if not ready:
                inm[b], outm[b], carry[b] = inflow, outflow, keep
            gl[b, 0], gl[b, 1], gl[b, 2] = gq, gk, gv
            lst[b], rst[b] = ls, rs

    def c_begin():
        for copy in own_slices:
            copy.wait()
        arrived_rows(7 * 16, z_recv.at[0])
        c_own()

    def c_share():
        c_end()
        for i in (0, 1):
            view = ct.at[2 * i : 2 * i + 2, :, c]
            send(1, view, view, d_recv.at[i], partner)

    def block(j):
        return (z * 2 + 10 + j) % 16

    def forward(j, state):
        b = block(j)
        inc[b] = state.astype(BF16)
        return carry[b][0:1] * state + lst[b]

    def backward(i, state):
        b = block(29 - i)
        ret[b] = state.astype(BF16)
        return carry[b][0:1] * state + rst[b]

    def finish(start, count):
        def run(i, carry_):
            done = []
            for b in [block(start + count * i + j) for j in range(count)]:
                inflow, outflow = inm[b], outm[b]
                done.append((b, (
                    gl[b, 0] + inflow * dot(upb[b, 0:128], inc[b], 1, 1),
                    gl[b, 1] + outflow * dot(part(b, 2), ret[b], 1, 1),
                    gl[b, 2] + outflow * dot(part(b, 1), ret[b], 1, 0),
                )))
            for b, parts in done:
                for k, value in enumerate(parts):
                    grads[b // 2, b % 2, :, 128 * k : 128 * (k + 1)] = value.astype(BF16)
            return carry_
        return run

    last = (zs[4] * 2, zs[4] * 2 + 1)
    attend((seq, z * 2 + other))
    up_hop(3)
    for d in (1, 2, 3):
        g_hop(d, 0, 0)
        g_hop(d, 0, 1)
        if d == 1:
            c_begin()
        if d == 2:
            c_mid()
        attend((below(d, 0), above(d, 0)))
        if d == 3:
            up_hop(4)
            prepare(last)
        g_hop(d, 1, 0)
        g_hop(d, 1, 1)
        attend((below(d, 1), above(d, 1)))
    c_share()
    zero = jnp.zeros((128, 128), F32)
    state_in = lax.fori_loop(0, 10, forward, zero)
    state_back = lax.fori_loop(0, 10, backward, zero)
    finish(4, 6)(0, 0)
    g_hop(4, 0, 0)
    g_hop(4, 0, 1)
    attend(last, ready=True)
    lax.fori_loop(10, 20, forward, state_in)
    lax.fori_loop(10, 20, backward, state_back)
    lax.fori_loop(0, 2, finish(10, 5), 0)
    def rows_of(core, parity):
        right = grads[:, parity].reshape(1024, 384)
        left = jnp.concatenate([ct[2 * core + j, :, parity].reshape(1024, 128) for j in (0, 1)], axis=1)
        return dot(left, right, 0, 0)

    rows_a[...] = rows_of(other, c)
    for i in (0, 1):
        arrived(ct.at[2 * i : 2 * i + 2, :, other], d_recv.at[i])
    rows_x[...] = (rows_a[...] + rows_of(other, other)).astype(BF16)
    send(3, rows_x, rows_r, o_recv.at[0], partner)
    mine = (rows_of(c, c) + rows_of(c, other)).astype(BF16)
    for i in range(3):
        out[i, :, lanes(c)] = mine[:, 128 * i : 128 * (i + 1)]
    arrived(rows_r, o_recv.at[0])
    for i in range(3):
        out[i, :, lanes(other)] = rows_r[:, 128 * i : 128 * (i + 1)]
    for kind, rows in sent.items():
        view = upb.at[0:15] if kind == 2 else w_all.at[0, 0:rows]
        pltpu.make_async_remote_copy(
            src_ref=view, dst_ref=view, send_sem=sends.at[kind], recv_sem=loc.at[0], device_id=partner, device_id_type=MESH
        ).wait_send()


def local(tokens, w_query, w_key, w_value, upstream, log_decay, segment):
    hbm = pl.BlockSpec(memory_space=pltpu.HBM)
    dma = pltpu.SemaphoreType.DMA
    out = pl.pallas_call(
        kernel,
        out_shape=jax.ShapeDtypeStruct((3, 256, 256), BF16),
        in_specs=[hbm] * 8,
        out_specs=pl.BlockSpec(memory_space=pltpu.VMEM),
        scratch_shapes=[
            pltpu.VMEM((2, 128), F32),
            pltpu.VMEM((16, 128), jnp.int32),
            pltpu.SMEM((2048,), jnp.int32),
            pltpu.VMEM((16, 128, 256), BF16),
            pltpu.VMEM((3, 4096, 256), BF16),
            pltpu.VMEM((16, 2, 3, 64, 128), BF16),
            pltpu.VMEM((2, 3, 64, 128), BF16),
            pltpu.VMEM((16, 136, 128), BF16),
            pltpu.VMEM((136, 128), BF16),
            pltpu.VMEM((4, 8, 2, 2, 4, 16, 128), BF16),
            pltpu.VMEM((16, 3, 128, 128), F32),
            pltpu.VMEM((16, 128, 128), F32),
            pltpu.VMEM((16, 128, 128), F32),
            pltpu.VMEM((16, 8, 128), F32),
            pltpu.VMEM((2, 128, 128), F32),
            pltpu.VMEM((16, 128, 128), F32),
            pltpu.VMEM((16, 128, 128), F32),
            pltpu.VMEM((16, 128, 128), BF16),
            pltpu.VMEM((16, 128, 128), BF16),
            pltpu.VMEM((8, 2, 128, 384), BF16),
            pltpu.VMEM((256, 384), F32),
            pltpu.VMEM((256, 384), BF16),
            pltpu.VMEM((256, 384), BF16),
            dma((2, 2, 3)), dma((2,)),
            dma((1,)), dma(()),
            dma((1,)), dma((9,)),
            dma((2,)), dma((32,)),
            dma((2,)), dma((1,)),
            dma((4,)), dma((8,)),
            pltpu.SemaphoreType.REGULAR((2,)),
        ],
        compiler_params=pltpu.CompilerParams(
            collective_id=0, has_side_effects=True, vmem_limit_bytes=40 * 1024 * 1024
        ),
    )(*[
        pltpu.with_memory_space_constraint(a, pltpu.HBM)
        for a in (
            tokens, w_query, w_key, w_value, upstream,
            log_decay.T, segment.reshape(16, 128), segment,
        )
    ])
    return out[0], out[1], out[2]


def solution(mesh):
    in_specs = (
        P("seq", "head"), P(None, "head"), P(None, "head"), P(None, "head"),
        P("seq", "head"), P("seq", "head"), P(),
    )
    out_specs = (P("seq", "head"),) * 3
    return jax.shard_map(local, mesh=mesh, in_specs=in_specs, out_specs=out_specs, check_vma=False)
```

```python
import jax
import jax.numpy as jnp
from jax import lax
from jax.experimental import pallas as pl
from jax.experimental.pallas import tpu as pltpu
from jax.sharding import PartitionSpec as P

HEAD = 128
SCALE = HEAD ** (-0.5)
MESH = pl.DeviceIdType.MESH
BF16, F32 = jnp.bfloat16, jnp.float32
AROUND = (1, 3, 2)


def dot(a, b, da, db):
    return lax.dot_general(a, b, (((da,), (db,)), ((), ())), preferred_element_type=F32)


def kernel(
    tok, wq, wk, wv, up, ldt_in, segv_in, segs_in,
    out,
    ldt, segv, segs, x_all, w_all, qkv, qkv_x, upb, up_x, ct,
    gl, inm, outm, carry, dec, lst, rst, inc, ret, grads, rows_x, rows_r,
    x_first, x_rest, c_first, c_rest, z_recv, u_recv, g_mate, g_recv, d_recv, o_recv, sends, loc, alive,
):
    seq, head = lax.axis_index("seq"), lax.axis_index("head")
    z, c = seq // 2, seq % 2
    x, y = head // 4, head % 4
    other = 1 - c
    zs = [(z + i) % 8 for i in range(8)]

    def plane_at(dx, dy):
        return ((x + dx) % 4) * 4 + (y + dy) % 4

    def at(dz=0, dx=0, dy=0, core=None):
        return {"seq": zs[dz] * 2 + (c if core is None else core), "head": plane_at(dx, dy)}

    partner = at(core=other)
    barrier = pltpu.get_barrier_semaphore()
    near = [partner] + [at(dx=i) for i in AROUND] + [at(dy=i) for i in AROUND] + [at(dz=i, core=j) for i in (1, 7) for j in (c, other)]
    for dev in near:
        pl.semaphore_signal(barrier, inc=1, device_id=dev, device_id_type=MESH)

    def fetch(src, dst, i):
        copy = pltpu.make_async_copy(src, dst, loc.at[i])
        copy.start()
        return copy

    def lanes(i):
        return pl.ds(pl.multiple_of(i * 128, 128), 128)

    own_tok = fetch(tok, x_all.at[head], 0)
    own_ldt = fetch(ldt_in, ldt, 2)
    own_up = fetch(up.at[:, lanes(c)], upb.at[seq, 0:128], 3)
    oth_up = fetch(up.at[:, lanes(other)], up_x.at[0:128], 4)
    seg_v = fetch(segv_in, segv, 5)
    seg_s = fetch(segs_in, segs, 6)
    for i, w in enumerate((wq, wk, wv)):
        fetch(w, w_all.at[i], 7)

    own_tok.wait()
    pl.semaphore_wait(barrier, len(near))
    for i in (1, 7):
        pl.semaphore_signal(alive.at[0], inc=1, device_id=at(dz=i), device_id_type=MESH)

    sent = {}

    def send(kind, src, dst, recv, dev):
        rows = src.dtype.itemsize
        for n in src.shape:
            rows *= n
        sent[kind] = sent.get(kind, 0) + rows // 512
        pltpu.make_async_remote_copy(
            src_ref=src, dst_ref=dst, send_sem=sends.at[kind], recv_sem=recv, device_id=dev, device_id_type=MESH
        ).start()

    def described(view, recv):
        return pltpu.make_async_remote_copy(
            src_ref=view, dst_ref=view, send_sem=sends.at[0], recv_sem=recv, device_id=partner, device_id_type=MESH
        )

    def arrived(view, recv):
        described(view, recv).wait_recv()

    def arrived_rows(rows, recv):
        arrived(w_all.at[0, 0:rows], recv)

    def plane(kind, unit, rows, first, rest, together=False):
        def there(half, stage, d):
            return at(dx=d) if half == stage else at(dy=d)

        def own():
            for half in (0, 1):
                for j, d in enumerate(AROUND):
                    view = unit(head, half)
                    send(kind, view, view, first.at[0] if together else first.at[half, j], there(half, 0, d))
            for half in (0, 1):
                for d in AROUND:
                    view = unit(head, half)
                    send(kind, view, view, rest, there(half, 1, d))

        def middle():
            if together:
                arrived_rows(6 * rows, first.at[0])
            for j, d in enumerate(AROUND):
                for half in (0, 1):
                    view = unit(plane_at(-d, 0) if half == 0 else plane_at(0, -d), half)
                    if not together:
                        arrived(view, first.at[half, j])
                    for e in AROUND:
                        send(kind, view, view, rest, there(half, 1, e))

        def end():
            arrived_rows(24 * rows, rest)

        return own, middle, end

    def x_unit(k):
        return lambda h, half: x_all.at[h, 64 * k + 32 * half : 64 * k + 32 * (half + 1)]

    def c_unit(h, half):
        return ct.at[h // 4, 4 * half : 4 * (half + 1), c, :, h % 4]

    def up_own():
        send(2, up_x, upb.at[seq], u_recv.at[8], partner)
        for i, j in ((1, 0), (7, 4)):
            send(2, upb.at[seq], upb.at[seq], u_recv.at[j], at(dz=i))
            send(2, up_x, upb.at[seq], u_recv.at[j], at(dz=i, core=other))

    def up_two():
        pl.semaphore_wait(alive.at[0], 2)
        for i in (2, 6):
            pl.semaphore_signal(alive.at[1], inc=1, device_id=at(dz=i), device_id_type=MESH)
        for i, j in ((2, 1), (6, 5)):
            send(2, upb.at[seq], upb.at[seq], u_recv.at[j], at(dz=i))
            send(2, up_x, upb.at[seq], u_recv.at[j], at(dz=i, core=other))

    def up_hop(d):
        below_, above_ = zs[8 - d] * 2, zs[d] * 2
        count = 2 if d < 4 else 1
        arrived(upb.at[0:count], u_recv.at[d - 1])
        if d in (2, 3):
            for parity in (c, other) if d < 3 else (c,):
                send(2, upb.at[below_ + parity], upb.at[below_ + parity], u_recv.at[d], at(dz=1))
        arrived(upb.at[0:count], u_recv.at[4 + d - 1])
        if d in (2, 3):
            for parity in (c, other) if d < 3 else (other,):
                send(2, upb.at[above_ + parity], upb.at[above_ + parity], u_recv.at[4 + d], at(dz=7))

    def g_send(src, s, k, down, d, p, core):
        send(3, src, qkv.at[s, k], g_recv.at[((down * 4 + d) * 2 + p) * 2 + k], at(dz=7 if down else 1, core=core))

    def g_own_first(k):
        g_send(qkv.at[seq, k], seq, k, 0, 0, 0, c)
        g_send(qkv_x.at[k], seq, k, 1, 0, 1, other)
        send(3, qkv_x.at[k], qkv.at[seq, k], g_mate.at[k], partner)

    def g_own_second(k):
        g_send(qkv_x.at[k], seq, k, 0, 0, 1, other)
        g_send(qkv.at[seq, k], seq, k, 1, 0, 0, c)

    def g_from_mate():
        for k in (0, 1):
            arrived(qkv.at[z * 2 + other, k], g_mate.at[k])
        arrived(upb.at[z * 2 + other], u_recv.at[8])

    def below(d, p):
        return zs[8 - d] * 2 + (c if p == 0 else other)

    def above(d, p):
        return zs[d] * 2 + (other if p == 0 else c)

    def g_hop(d, p, k):
        for down, s, q in ((0, below(d, p), p), (1, above(d, p), 1 - p)):
            arrived(qkv.at[s, k], g_recv.at[((down * 4 + d - 1) * 2 + q) * 2 + k])
            if d < 3 or (d == 3 and p == 0):
                g_send(qkv.at[s, k], s, k, down, d, q, c)

    def project(k):
        for i in range(3):
            acc = dot(x_all[0, 64 * k : 64 * (k + 1)], w_all[i, 0:256, :], 1, 0)
            for h in range(1, 16):
                acc = acc + dot(x_all[h, 64 * k : 64 * (k + 1)], w_all[i, 256 * h : 256 * (h + 1), :], 1, 0)
            acc = acc.astype(BF16)
            qkv[seq, k, i] = jnp.where(c == 0, acc[:, :128], acc[:, 128:])
            qkv_x[k, i] = jnp.where(c == 0, acc[:, 128:], acc[:, :128])

    quarter, group = head // 4, head % 4

    def slice_of(zt, k):
        rows = pl.ds(pl.multiple_of(64 * k + 16 * group, 16), 16)
        return x_all.at[2 * zt + quarter // 2, rows, lanes(quarter % 2)]

    own_slices = []

    def slices_out(k):
        own_slices.append(fetch(slice_of(z, k), ct.at[quarter, z, c, k, group], k))
        for i in (4, 3, 5, 2, 6, 1, 7):
            send(3, slice_of(zs[i], k), ct.at[quarter, z, c, k, group], z_recv.at[0], at(dz=i))

    a_own, a_mid, a_end = zip(*[plane(0, x_unit(k), 32, x_first.at[k], x_rest.at[k]) for k in (0, 1)])
    c_own, c_mid, c_end = plane(0, c_unit, 64, c_first, c_rest, together=True)

    a_own[0]()

    own_ldt.wait()
    total = jnp.concatenate([ldt[...], jnp.zeros((6, 128), F32)], axis=0)
    lane = lax.broadcasted_iota(jnp.int32, (8, 128), 1)
    for k in (1, 2, 4, 8, 16, 32, 64):
        total = total + jnp.where(lane >= k, pltpu.roll(total, k, 1), 0.0)

    def in_parts(row):
        hi = row.astype(BF16)
        rest = row - hi.astype(F32)
        mid = rest.astype(BF16)
        low = (rest - mid.astype(F32)).astype(BF16)
        return jnp.concatenate([hi.astype(F32), mid.astype(F32), low.astype(F32), jnp.zeros((5, 128), F32)], axis=0).astype(BF16)

    lo, hi = in_parts(total[0:1]), in_parts(total[1:2])
    upb[seq, 128:136] = jnp.where(c == 0, lo, hi)
    up_x[128:136] = jnp.where(c == 0, hi, lo)

    own_up.wait()
    oth_up.wait()
    a_own[1]()
    up_own()
    up_two()
    a_mid[0]()
    a_mid[1]()
    up_hop(1)
    pl.when(c == 0)(lambda: up_hop(2))
    pltpu.make_async_copy(w_all, w_all, loc.at[7]).wait()
    seg_v.wait()
    seg_s.wait()
    a_end[0]()
    pl.semaphore_wait(alive.at[1], 2)
    slices_out(0)
    project(0)
    g_own_first(0)
    pl.when(c == 1)(lambda: up_hop(2))
    a_end[1]()

    slices_out(1)
    project(1)
    g_own_first(1)
    g_own_second(0)
    g_own_second(1)
    g_from_mate()

    ti = lax.broadcasted_iota(jnp.int32, (128, 128), 0)
    si = lax.broadcasted_iota(jnp.int32, (128, 128), 1)

    def part(b, i):
        return jnp.concatenate([qkv[b, 0, i], qkv[b, 1, i]], axis=0)

    def prepared(b):
        parts = upb[b, 128:136].astype(F32)
        row = parts[0:1] + parts[1:2] + parts[2:3]
        before = segs[jnp.maximum(b * 128 - 1, 0)]
        previous = jnp.where(b > 0, before, -1).astype(F32)
        last = segs[b * 128 + 127].astype(F32)
        ls_s = jnp.broadcast_to(row, (128, 128))
        ls_t = ls_s.T
        seg_s = jnp.broadcast_to(segv[pl.ds(b, 1), :], (128, 128)).astype(F32)
        seg_t = seg_s.T
        same = (seg_s == seg_t) & (ti >= si)
        decay = jnp.where(same, SCALE * jnp.exp(jnp.where(same, ls_t - ls_s, 0.0)), 0.0)
        ls_last = row[:, 127:128]
        inflow = jnp.where(seg_t == previous, jnp.exp(ls_t), 0.0)
        outflow = jnp.where(seg_t == last, jnp.exp(ls_last - ls_t), 0.0)
        keep = jnp.where(last == previous, jnp.exp(ls_last), 0.0)
        return decay, inflow, outflow, jnp.broadcast_to(keep, (8, 128))

    def prepare(blocks):
        for j, b in enumerate(blocks):
            dec[j], inm[b], outm[b], carry[b] = prepared(b)

    def attend(blocks, ready=False):
        done = []
        for j, b in enumerate(blocks):
            q, k, v, u = part(b, 0), part(b, 1), part(b, 2), upb[b, 0:128]
            if ready:
                decay, inflow, outflow, keep = dec[j], inm[b], outm[b], None
            else:
                decay, inflow, outflow, keep = prepared(b)
            a_qk = (decay * dot(q, k, 1, 1)).astype(BF16)
            a_up = (decay * dot(u, v, 1, 1)).astype(BF16)
            wk_ = (SCALE * outflow * k.astype(F32)).astype(BF16)
            wq_ = (SCALE * inflow * q.astype(F32)).astype(BF16)
            done.append((
                inflow, outflow, keep, dot(a_up, k, 1, 0), dot(a_up, q, 0, 0),
                dot(a_qk, u, 0, 0), dot(wk_, v, 0, 0), dot(wq_, u, 0, 0),
            ))
        for b, (inflow, outflow, keep, gq, gk, gv, ls, rs) in zip(blocks, done):
            if not ready:
                inm[b], outm[b], carry[b] = inflow, outflow, keep
            gl[b, 0], gl[b, 1], gl[b, 2] = gq, gk, gv
            lst[b], rst[b] = ls, rs

    def c_begin():
        for copy in own_slices:
            copy.wait()
        arrived_rows(7 * 16, z_recv.at[0])
        c_own()

    def c_share():
        c_end()
        for i in (0, 1):
            view = ct.at[2 * i : 2 * i + 2, :, c]
            send(1, view, view, d_recv.at[i], partner)

    def block(j):
        return (z * 2 + 10 + j) % 16

    def scan(i, states):
        ahead, back = states
        b, e = block(i), block(29 - i)
        inc[b], ret[e] = ahead.astype(BF16), back.astype(BF16)
        return carry[b][0:1] * ahead + lst[b], carry[e][0:1] * back + rst[e]

    def finish(start, count):
        def run(i, carry_):
            done = []
            for b in [block(start + count * i + j) for j in range(count)]:
                inflow, outflow = inm[b], outm[b]
                done.append((b, (
                    gl[b, 0] + inflow * dot(upb[b, 0:128], inc[b], 1, 1),
                    gl[b, 1] + outflow * dot(part(b, 2), ret[b], 1, 1),
                    gl[b, 2] + outflow * dot(part(b, 1), ret[b], 1, 0),
                )))
            for b, parts in done:
                for k, value in enumerate(parts):
                    grads[b // 2, b % 2, :, 128 * k : 128 * (k + 1)] = value.astype(BF16)
            return carry_
        return run

    last = (zs[4] * 2, zs[4] * 2 + 1)
    attend((seq, z * 2 + other))
    up_hop(3)
    for d in (1, 2, 3):
        g_hop(d, 0, 0)
        g_hop(d, 0, 1)
        if d == 1:
            c_begin()
        if d == 2:
            c_mid()
        attend((below(d, 0), above(d, 0)))
        if d == 3:
            up_hop(4)
            prepare(last)
        g_hop(d, 1, 0)
        g_hop(d, 1, 1)
        if d == 3:
            c_share()
        attend((below(d, 1), above(d, 1)))
    zero = jnp.zeros((128, 128), F32)
    states = lax.fori_loop(0, 10, scan, (zero, zero), unroll=5)
    finish(4, 6)(0, 0)
    g_hop(4, 0, 0)
    g_hop(4, 0, 1)
    attend(last, ready=True)
    lax.fori_loop(10, 20, scan, states, unroll=5)
    lax.fori_loop(0, 2, finish(10, 5), 0)
    def rows_of(core):
        left = jnp.concatenate([ct[2 * core + j].reshape(2048, 128) for j in (0, 1)], axis=1)
        return dot(left, grads[...].reshape(2048, 384), 0, 0).astype(BF16)

    for i in (0, 1):
        arrived(ct.at[2 * i : 2 * i + 2, :, other], d_recv.at[i])
    rows_x[...] = rows_of(other)
    send(3, rows_x, rows_r, o_recv.at[0], partner)
    mine = rows_of(c)
    for i in range(3):
        out[i, :, lanes(c)] = mine[:, 128 * i : 128 * (i + 1)]
    arrived(rows_r, o_recv.at[0])
    for i in range(3):
        out[i, :, lanes(other)] = rows_r[:, 128 * i : 128 * (i + 1)]
    for kind, rows in sent.items():
        view = upb.at[0:15] if kind == 2 else w_all.at[0, 0:rows]
        pltpu.make_async_remote_copy(
            src_ref=view, dst_ref=view, send_sem=sends.at[kind], recv_sem=loc.at[0], device_id=partner, device_id_type=MESH
        ).wait_send()


def local(tokens, w_query, w_key, w_value, upstream, log_decay, segment):
    hbm = pl.BlockSpec(memory_space=pltpu.HBM)
    dma = pltpu.SemaphoreType.DMA
    out = pl.pallas_call(
        kernel,
        out_shape=jax.ShapeDtypeStruct((3, 256, 256), BF16),
        in_specs=[hbm] * 8,
        out_specs=pl.BlockSpec(memory_space=pltpu.VMEM),
        scratch_shapes=[
            pltpu.VMEM((2, 128), F32),
            pltpu.VMEM((16, 128), jnp.int32),
            pltpu.SMEM((2048,), jnp.int32),
            pltpu.VMEM((16, 128, 256), BF16),
            pltpu.VMEM((3, 4096, 256), BF16),
            pltpu.VMEM((16, 2, 3, 64, 128), BF16),
            pltpu.VMEM((2, 3, 64, 128), BF16),
            pltpu.VMEM((16, 136, 128), BF16),
            pltpu.VMEM((136, 128), BF16),
            pltpu.VMEM((4, 8, 2, 2, 4, 16, 128), BF16),
            pltpu.VMEM((16, 3, 128, 128), F32),
            pltpu.VMEM((16, 128, 128), F32),
            pltpu.VMEM((16, 128, 128), F32),
            pltpu.VMEM((16, 8, 128), F32),
            pltpu.VMEM((2, 128, 128), F32),
            pltpu.VMEM((16, 128, 128), F32),
            pltpu.VMEM((16, 128, 128), F32),
            pltpu.VMEM((16, 128, 128), BF16),
            pltpu.VMEM((16, 128, 128), BF16),
            pltpu.VMEM((8, 2, 128, 384), BF16),
            pltpu.VMEM((256, 384), BF16),
            pltpu.VMEM((256, 384), BF16),
            dma((2, 2, 3)), dma((2,)),
            dma((1,)), dma(()),
            dma((1,)), dma((9,)),
            dma((2,)), dma((32,)),
            dma((2,)), dma((1,)),
            dma((4,)), dma((8,)),
            pltpu.SemaphoreType.REGULAR((2,)),
        ],
        compiler_params=pltpu.CompilerParams(
            collective_id=0, has_side_effects=True, vmem_limit_bytes=40 * 1024 * 1024
        ),
    )(*[
        pltpu.with_memory_space_constraint(a, pltpu.HBM)
        for a in (
            tokens, w_query, w_key, w_value, upstream,
            log_decay.T, segment.reshape(16, 128), segment,
        )
    ])
    return out[0], out[1], out[2]


def solution(mesh):
    in_specs = (
        P("seq", "head"), P(None, "head"), P(None, "head"), P(None, "head"),
        P("seq", "head"), P("seq", "head"), P(),
    )
    out_specs = (P("seq", "head"),) * 3
    return jax.shard_map(local, mesh=mesh, in_specs=in_specs, out_specs=out_specs, check_vma=False)
```

```python
import jax
import jax.numpy as jnp
from jax import lax
from jax.experimental import pallas as pl
from jax.experimental.pallas import tpu as pltpu
from jax.sharding import PartitionSpec as P

HEAD = 128
SCALE = HEAD ** (-0.5)
MESH = pl.DeviceIdType.MESH
BF16, F32 = jnp.bfloat16, jnp.float32
AROUND = (1, 3, 2)


def dot(a, b, da, db):
    return lax.dot_general(a, b, (((da,), (db,)), ((), ())), preferred_element_type=F32)


def kernel(
    tok, wq, wk, wv, up, ldt_in, segv_in, segs_in,
    out,
    ldt, segv, segs, x_all, w_all, qkv, qkv_x, upb, up_x, ct,
    gl, inm, outm, carry, dec, lst, rst, inc, ret, grads, rows_x, rows_r,
    x_first, x_rest, c_first, c_rest, z_recv, u_recv, g_mate, g_recv, d_recv, o_recv, sends, loc, alive,
):
    seq, head = lax.axis_index("seq"), lax.axis_index("head")
    z, c = seq // 2, seq % 2
    x, y = head // 4, head % 4
    other = 1 - c
    zs = [(z + i) % 8 for i in range(8)]

    def plane_at(dx, dy):
        return ((x + dx) % 4) * 4 + (y + dy) % 4

    def at(dz=0, dx=0, dy=0, core=None):
        return {"seq": zs[dz] * 2 + (c if core is None else core), "head": plane_at(dx, dy)}

    partner = at(core=other)
    barrier = pltpu.get_barrier_semaphore()
    near = [partner] + [at(dx=i) for i in AROUND] + [at(dy=i) for i in AROUND] + [at(dz=i, core=j) for i in (1, 7) for j in (c, other)]
    for dev in near:
        pl.semaphore_signal(barrier, inc=1, device_id=dev, device_id_type=MESH)

    def fetch(src, dst, i):
        copy = pltpu.make_async_copy(src, dst, loc.at[i])
        copy.start()
        return copy

    def lanes(i):
        return pl.ds(pl.multiple_of(i * 128, 128), 128)

    own_tok = fetch(tok, x_all.at[head], 0)
    own_ldt = fetch(ldt_in, ldt, 2)
    own_up = fetch(up.at[:, lanes(c)], upb.at[seq, 0:128], 3)
    oth_up = fetch(up.at[:, lanes(other)], up_x.at[0:128], 4)
    seg_v = fetch(segv_in, segv, 5)
    seg_s = fetch(segs_in, segs, 6)
    for i, w in enumerate((wq, wk, wv)):
        fetch(w, w_all.at[i], 7)

    own_tok.wait()
    pl.semaphore_wait(barrier, len(near))
    for i in (1, 7):
        pl.semaphore_signal(alive.at[0], inc=1, device_id=at(dz=i), device_id_type=MESH)

    sent = {}

    def send(kind, src, dst, recv, dev):
        rows = src.dtype.itemsize
        for n in src.shape:
            rows *= n
        sent[kind] = sent.get(kind, 0) + rows // 512
        pltpu.make_async_remote_copy(
            src_ref=src, dst_ref=dst, send_sem=sends.at[kind], recv_sem=recv, device_id=dev, device_id_type=MESH
        ).start()

    def described(view, recv):
        return pltpu.make_async_remote_copy(
            src_ref=view, dst_ref=view, send_sem=sends.at[0], recv_sem=recv, device_id=partner, device_id_type=MESH
        )

    def arrived(view, recv):
        described(view, recv).wait_recv()

    def arrived_rows(rows, recv):
        arrived(w_all.at[0, 0:rows], recv)

    def plane(kind, unit, rows, first, rest, together=False):
        def there(half, stage, d):
            return at(dx=d) if half == stage else at(dy=d)

        def own():
            for half in (0, 1):
                for j, d in enumerate(AROUND):
                    view = unit(head, half)
                    send(kind, view, view, first.at[0] if together else first.at[half, j], there(half, 0, d))
            for half in (0, 1):
                for d in AROUND:
                    view = unit(head, half)
                    send(kind, view, view, rest, there(half, 1, d))

        def middle():
            if together:
                arrived_rows(6 * rows, first.at[0])
            for j, d in enumerate(AROUND):
                for half in (0, 1):
                    view = unit(plane_at(-d, 0) if half == 0 else plane_at(0, -d), half)
                    if not together:
                        arrived(view, first.at[half, j])
                    for e in AROUND:
                        send(kind, view, view, rest, there(half, 1, e))

        def end():
            arrived_rows(24 * rows, rest)

        return own, middle, end

    def x_unit(k):
        return lambda h, half: x_all.at[h, 64 * k + 32 * half : 64 * k + 32 * (half + 1)]

    def c_unit(h, half):
        return ct.at[h // 4, 4 * half : 4 * (half + 1), c, :, h % 4]

    def up_own():
        send(2, up_x, upb.at[seq], u_recv.at[8], partner)
        for i, j in ((1, 0), (7, 4)):
            send(2, upb.at[seq], upb.at[seq], u_recv.at[j], at(dz=i))
            send(2, up_x, upb.at[seq], u_recv.at[j], at(dz=i, core=other))

    def up_two():
        pl.semaphore_wait(alive.at[0], 2)
        for i in (2, 6):
            pl.semaphore_signal(alive.at[1], inc=1, device_id=at(dz=i), device_id_type=MESH)
        for i, j in ((2, 1), (6, 5)):
            send(2, upb.at[seq], upb.at[seq], u_recv.at[j], at(dz=i))
            send(2, up_x, upb.at[seq], u_recv.at[j], at(dz=i, core=other))

    def up_hop(d):
        below_, above_ = zs[8 - d] * 2, zs[d] * 2
        count = 2 if d < 4 else 1
        arrived(upb.at[0:count], u_recv.at[d - 1])
        if d in (2, 3):
            for parity in (c, other) if d < 3 else (c,):
                send(2, upb.at[below_ + parity], upb.at[below_ + parity], u_recv.at[d], at(dz=1))
        arrived(upb.at[0:count], u_recv.at[4 + d - 1])
        if d in (2, 3):
            for parity in (c, other) if d < 3 else (other,):
                send(2, upb.at[above_ + parity], upb.at[above_ + parity], u_recv.at[4 + d], at(dz=7))

    def g_send(src, s, k, down, d, p, core):
        send(3, src, qkv.at[s, k], g_recv.at[((down * 4 + d) * 2 + p) * 2 + k], at(dz=7 if down else 1, core=core))

    def g_own_first(k):
        g_send(qkv.at[seq, k], seq, k, 0, 0, 0, c)
        g_send(qkv_x.at[k], seq, k, 1, 0, 1, other)
        send(3, qkv_x.at[k], qkv.at[seq, k], g_mate.at[k], partner)

    def g_own_second(k):
        g_send(qkv_x.at[k], seq, k, 0, 0, 1, other)
        g_send(qkv.at[seq, k], seq, k, 1, 0, 0, c)

    def g_from_mate():
        for k in (0, 1):
            arrived(qkv.at[z * 2 + other, k], g_mate.at[k])
        arrived(upb.at[z * 2 + other], u_recv.at[8])

    def below(d, p):
        return zs[8 - d] * 2 + (c if p == 0 else other)

    def above(d, p):
        return zs[d] * 2 + (other if p == 0 else c)

    def g_hop(d, p, k):
        for down, s, q in ((0, below(d, p), p), (1, above(d, p), 1 - p)):
            arrived(qkv.at[s, k], g_recv.at[((down * 4 + d - 1) * 2 + q) * 2 + k])
            if d < 3 or (d == 3 and p == 0):
                g_send(qkv.at[s, k], s, k, down, d, q, c)

    def project(k):
        for i in range(3):
            acc = dot(x_all[0, 64 * k : 64 * (k + 1)], w_all[i, 0:256, :], 1, 0)
            for h in range(1, 16):
                acc = acc + dot(x_all[h, 64 * k : 64 * (k + 1)], w_all[i, 256 * h : 256 * (h + 1), :], 1, 0)
            acc = acc.astype(BF16)
            qkv[seq, k, i] = jnp.where(c == 0, acc[:, :128], acc[:, 128:])
            qkv_x[k, i] = jnp.where(c == 0, acc[:, 128:], acc[:, :128])

    quarter, group = head // 4, head % 4

    def slice_of(zt, k):
        rows = pl.ds(pl.multiple_of(64 * k + 16 * group, 16), 16)
        return x_all.at[2 * zt + quarter // 2, rows, lanes(quarter % 2)]

    own_slices = []

    def slices_out(k):
        own_slices.append(fetch(slice_of(z, k), ct.at[quarter, z, c, k, group], k))
        for i in (4, 3, 5, 2, 6, 1, 7):
            send(3, slice_of(zs[i], k), ct.at[quarter, z, c, k, group], z_recv.at[0], at(dz=i))

    a_own, a_mid, a_end = zip(*[plane(0, x_unit(k), 32, x_first.at[k], x_rest.at[k]) for k in (0, 1)])
    c_own, c_mid, c_end = plane(0, c_unit, 64, c_first, c_rest, together=True)

    a_own[0]()

    own_ldt.wait()
    total = jnp.concatenate([ldt[...], jnp.zeros((6, 128), F32)], axis=0)
    lane = lax.broadcasted_iota(jnp.int32, (8, 128), 1)
    for k in (1, 2, 4, 8, 16, 32, 64):
        total = total + jnp.where(lane >= k, pltpu.roll(total, k, 1), 0.0)

    def in_parts(row):
        hi = row.astype(BF16)
        rest = row - hi.astype(F32)
        mid = rest.astype(BF16)
        low = (rest - mid.astype(F32)).astype(BF16)
        return jnp.concatenate([hi.astype(F32), mid.astype(F32), low.astype(F32), jnp.zeros((5, 128), F32)], axis=0).astype(BF16)

    lo, hi = in_parts(total[0:1]), in_parts(total[1:2])
    upb[seq, 128:136] = jnp.where(c == 0, lo, hi)
    up_x[128:136] = jnp.where(c == 0, hi, lo)

    own_up.wait()
    oth_up.wait()
    a_own[1]()
    up_own()
    up_two()
    a_mid[0]()
    a_mid[1]()
    up_hop(1)
    pl.when(c == 0)(lambda: up_hop(2))
    pltpu.make_async_copy(w_all, w_all, loc.at[7]).wait()
    seg_v.wait()
    seg_s.wait()
    a_end[0]()
    pl.semaphore_wait(alive.at[1], 2)
    slices_out(0)
    project(0)
    g_own_first(0)
    pl.when(c == 1)(lambda: up_hop(2))
    a_end[1]()

    slices_out(1)
    project(1)
    g_own_first(1)
    g_own_second(0)
    g_own_second(1)
    g_from_mate()

    ti = lax.broadcasted_iota(jnp.int32, (128, 128), 0)
    si = lax.broadcasted_iota(jnp.int32, (128, 128), 1)

    def part(b, i):
        return jnp.concatenate([qkv[b, 0, i], qkv[b, 1, i]], axis=0)

    def prepared(b):
        parts = upb[b, 128:136].astype(F32)
        row = parts[0:1] + parts[1:2] + parts[2:3]
        before = segs[jnp.maximum(b * 128 - 1, 0)]
        previous = jnp.where(b > 0, before, -1).astype(F32)
        last = segs[b * 128 + 127].astype(F32)
        ls_s = jnp.broadcast_to(row, (128, 128))
        ls_t = ls_s.T
        seg_s = jnp.broadcast_to(segv[pl.ds(b, 1), :], (128, 128)).astype(F32)
        seg_t = seg_s.T
        same = (seg_s == seg_t) & (ti >= si)
        decay = jnp.where(same, SCALE * jnp.exp(jnp.where(same, ls_t - ls_s, 0.0)), 0.0)
        ls_last = row[:, 127:128]
        inflow = jnp.where(seg_t == previous, jnp.exp(ls_t), 0.0)
        outflow = jnp.where(seg_t == last, jnp.exp(ls_last - ls_t), 0.0)
        keep = jnp.where(last == previous, jnp.exp(ls_last), 0.0)
        return decay, inflow, outflow, jnp.broadcast_to(keep, (8, 128))

    def prepare(blocks):
        for j, b in enumerate(blocks):
            dec[j], inm[b], outm[b], carry[b] = prepared(b)

    def attend(blocks, ready=False):
        done = []
        for j, b in enumerate(blocks):
            q, k, v, u = part(b, 0), part(b, 1), part(b, 2), upb[b, 0:128]
            if ready:
                decay, inflow, outflow, keep = dec[j], inm[b], outm[b], None
            else:
                decay, inflow, outflow, keep = prepared(b)
            a_qk = (decay * dot(q, k, 1, 1)).astype(BF16)
            a_up = (decay * dot(u, v, 1, 1)).astype(BF16)
            wk_ = (SCALE * outflow * k.astype(F32)).astype(BF16)
            wq_ = (SCALE * inflow * q.astype(F32)).astype(BF16)
            done.append((
                inflow, outflow, keep, dot(a_up, k, 1, 0), dot(a_up, q, 0, 0),
                dot(a_qk, u, 0, 0), dot(wk_, v, 0, 0), dot(wq_, u, 0, 0),
            ))
        for b, (inflow, outflow, keep, gq, gk, gv, ls, rs) in zip(blocks, done):
            if not ready:
                inm[b], outm[b], carry[b] = inflow, outflow, keep
            gl[b, 0], gl[b, 1], gl[b, 2] = gq, gk, gv
            lst[b], rst[b] = ls, rs

    def c_begin():
        for copy in own_slices:
            copy.wait()
        arrived_rows(7 * 16, z_recv.at[0])
        c_own()

    def c_share():
        c_end()
        for i in (0, 1):
            view = ct.at[2 * i : 2 * i + 2, :, c]
            send(1, view, view, d_recv.at[i], partner)

    def block(j):
        return (z * 2 + 10 + j) % 16

    def scan(i, states):
        ahead, back = states
        b, e = block(i), block(29 - i)
        inc[b], ret[e] = ahead.astype(BF16), back.astype(BF16)
        return carry[b][0:1] * ahead + lst[b], carry[e][0:1] * back + rst[e]

    def finish(start, count):
        def run(i, carry_):
            done = []
            for b in [block(start + count * i + j) for j in range(count)]:
                inflow, outflow = inm[b], outm[b]
                done.append((b, (
                    gl[b, 0] + inflow * dot(upb[b, 0:128], inc[b], 1, 1),
                    gl[b, 1] + outflow * dot(part(b, 2), ret[b], 1, 1),
                    gl[b, 2] + outflow * dot(part(b, 1), ret[b], 1, 0),
                )))
            for b, parts in done:
                for k, value in enumerate(parts):
                    grads[b // 2, b % 2, :, 128 * k : 128 * (k + 1)] = value.astype(BF16)
            return carry_
        return run

    last = (zs[4] * 2, zs[4] * 2 + 1)
    attend((seq, z * 2 + other))
    up_hop(3)
    for d in (1, 2, 3):
        g_hop(d, 0, 0)
        g_hop(d, 0, 1)
        if d == 1:
            c_begin()
        if d == 2:
            c_mid()
        attend((below(d, 0), above(d, 0)))
        if d == 3:
            up_hop(4)
            prepare(last)
        g_hop(d, 1, 0)
        g_hop(d, 1, 1)
        if d == 3:
            c_share()
        attend((below(d, 1), above(d, 1)))
    zero = jnp.zeros((128, 128), F32)
    states = lax.fori_loop(0, 10, scan, (zero, zero), unroll=5)
    finish(4, 6)(0, 0)
    g_hop(4, 0, 0)
    g_hop(4, 0, 1)
    attend(last, ready=True)
    lax.fori_loop(10, 20, scan, states, unroll=5)
    finish(10, 10)(0, 0)
    def rows_of(core):
        left = jnp.concatenate([ct[2 * core + j].reshape(2048, 128) for j in (0, 1)], axis=1)
        return dot(left, grads[...].reshape(2048, 384), 0, 0).astype(BF16)

    for i in (0, 1):
        arrived(ct.at[2 * i : 2 * i + 2, :, other], d_recv.at[i])
    rows_x[...] = rows_of(other)
    send(3, rows_x, rows_r, o_recv.at[0], partner)
    mine = rows_of(c)
    for i in range(3):
        out[i, :, lanes(c)] = mine[:, 128 * i : 128 * (i + 1)]
    arrived(rows_r, o_recv.at[0])
    for i in range(3):
        out[i, :, lanes(other)] = rows_r[:, 128 * i : 128 * (i + 1)]
    for kind, rows in sent.items():
        view = upb.at[0:15] if kind == 2 else w_all.at[0, 0:rows]
        pltpu.make_async_remote_copy(
            src_ref=view, dst_ref=view, send_sem=sends.at[kind], recv_sem=loc.at[0], device_id=partner, device_id_type=MESH
        ).wait_send()


def local(tokens, w_query, w_key, w_value, upstream, log_decay, segment):
    hbm = pl.BlockSpec(memory_space=pltpu.HBM)
    dma = pltpu.SemaphoreType.DMA
    out = pl.pallas_call(
        kernel,
        out_shape=jax.ShapeDtypeStruct((3, 256, 256), BF16),
        in_specs=[hbm] * 8,
        out_specs=pl.BlockSpec(memory_space=pltpu.VMEM),
        scratch_shapes=[
            pltpu.VMEM((2, 128), F32),
            pltpu.VMEM((16, 128), jnp.int32),
            pltpu.SMEM((2048,), jnp.int32),
            pltpu.VMEM((16, 128, 256), BF16),
            pltpu.VMEM((3, 4096, 256), BF16),
            pltpu.VMEM((16, 2, 3, 64, 128), BF16),
            pltpu.VMEM((2, 3, 64, 128), BF16),
            pltpu.VMEM((16, 136, 128), BF16),
            pltpu.VMEM((136, 128), BF16),
            pltpu.VMEM((4, 8, 2, 2, 4, 16, 128), BF16),
            pltpu.VMEM((16, 3, 128, 128), F32),
            pltpu.VMEM((16, 128, 128), F32),
            pltpu.VMEM((16, 128, 128), F32),
            pltpu.VMEM((16, 8, 128), F32),
            pltpu.VMEM((2, 128, 128), F32),
            pltpu.VMEM((16, 128, 128), F32),
            pltpu.VMEM((16, 128, 128), F32),
            pltpu.VMEM((16, 128, 128), BF16),
            pltpu.VMEM((16, 128, 128), BF16),
            pltpu.VMEM((8, 2, 128, 384), BF16),
            pltpu.VMEM((256, 384), BF16),
            pltpu.VMEM((256, 384), BF16),
            dma((2, 2, 3)), dma((2,)),
            dma((1,)), dma(()),
            dma((1,)), dma((9,)),
            dma((2,)), dma((32,)),
            dma((2,)), dma((1,)),
            dma((4,)), dma((8,)),
            pltpu.SemaphoreType.REGULAR((2,)),
        ],
        compiler_params=pltpu.CompilerParams(
            collective_id=0, has_side_effects=True, vmem_limit_bytes=40 * 1024 * 1024
        ),
    )(*[
        pltpu.with_memory_space_constraint(a, pltpu.HBM)
        for a in (
            tokens, w_query, w_key, w_value, upstream,
            log_decay.T, segment.reshape(16, 128), segment,
        )
    ])
    return out[0], out[1], out[2]


def solution(mesh):
    in_specs = (
        P("seq", "head"), P(None, "head"), P(None, "head"), P(None, "head"),
        P("seq", "head"), P("seq", "head"), P(),
    )
    out_specs = (P("seq", "head"),) * 3
    return jax.shard_map(local, mesh=mesh, in_specs=in_specs, out_specs=out_specs, check_vma=False)
```

```python
import jax
import jax.numpy as jnp
from jax import lax
from jax.experimental import pallas as pl
from jax.experimental.pallas import tpu as pltpu
from jax.sharding import PartitionSpec as P

HEAD = 128
SCALE = HEAD ** (-0.5)
MESH = pl.DeviceIdType.MESH
BF16, F32 = jnp.bfloat16, jnp.float32
AROUND = (1, 3, 2)


def dot(a, b, da, db):
    return lax.dot_general(a, b, (((da,), (db,)), ((), ())), preferred_element_type=F32)


def kernel(
    tok, wq, wk, wv, up, ldt_in, segv_in, segs_in,
    out,
    ldt, segv, segs, x_all, w_all, qkv, qkv_x, upb, up_x, ct,
    gl, inm, outm, carry, dec, lst, rst, inc, ret, grads, rows_x, rows_r,
    x_first, x_rest, c_first, c_rest, z_recv, u_recv, g_mate, g_recv, d_recv, o_recv, sends, loc, alive,
):
    seq, head = lax.axis_index("seq"), lax.axis_index("head")
    z, c = seq // 2, seq % 2
    x, y = head // 4, head % 4
    other = 1 - c
    zs = [(z + i) % 8 for i in range(8)]

    def plane_at(dx, dy):
        return ((x + dx) % 4) * 4 + (y + dy) % 4

    def at(dz=0, dx=0, dy=0, core=None):
        return {"seq": zs[dz] * 2 + (c if core is None else core), "head": plane_at(dx, dy)}

    partner = at(core=other)
    barrier = pltpu.get_barrier_semaphore()
    near = [partner] + [at(dx=i) for i in AROUND] + [at(dy=i) for i in AROUND] + [at(dz=i, core=j) for i in (1, 7) for j in (c, other)]
    for dev in near:
        pl.semaphore_signal(barrier, inc=1, device_id=dev, device_id_type=MESH)

    def fetch(src, dst, i):
        copy = pltpu.make_async_copy(src, dst, loc.at[i])
        copy.start()
        return copy

    def lanes(i):
        return pl.ds(pl.multiple_of(i * 128, 128), 128)

    own_tok = fetch(tok, x_all.at[head], 0)
    own_ldt = fetch(ldt_in, ldt, 2)
    own_up = fetch(up.at[:, lanes(c)], upb.at[seq, 0:128], 3)
    oth_up = fetch(up.at[:, lanes(other)], up_x.at[0:128], 4)
    seg_v = fetch(segv_in, segv, 5)
    seg_s = fetch(segs_in, segs, 6)
    for i, w in enumerate((wq, wk, wv)):
        fetch(w, w_all.at[i], 7)

    own_tok.wait()
    pl.semaphore_wait(barrier, len(near))
    for i in (1, 7):
        pl.semaphore_signal(alive.at[0], inc=1, device_id=at(dz=i), device_id_type=MESH)

    sent = {}

    def send(kind, src, dst, recv, dev):
        rows = src.dtype.itemsize
        for n in src.shape:
            rows *= n
        sent[kind] = sent.get(kind, 0) + rows // 512
        pltpu.make_async_remote_copy(
            src_ref=src, dst_ref=dst, send_sem=sends.at[kind], recv_sem=recv, device_id=dev, device_id_type=MESH
        ).start()

    def described(view, recv):
        return pltpu.make_async_remote_copy(
            src_ref=view, dst_ref=view, send_sem=sends.at[0], recv_sem=recv, device_id=partner, device_id_type=MESH
        )

    def arrived(view, recv):
        described(view, recv).wait_recv()

    def arrived_rows(rows, recv):
        arrived(w_all.at[0, 0:rows], recv)

    def plane(kind, unit, rows, first, rest, together=False):
        def there(half, stage, d):
            return at(dx=d) if half == stage else at(dy=d)

        def own():
            for half in (0, 1):
                for j, d in enumerate(AROUND):
                    view = unit(head, half)
                    send(kind, view, view, first.at[0] if together else first.at[half, j], there(half, 0, d))
            for half in (0, 1):
                for d in AROUND:
                    view = unit(head, half)
                    send(kind, view, view, rest, there(half, 1, d))

        def middle():
            if together:
                arrived_rows(6 * rows, first.at[0])
            for j, d in enumerate(AROUND):
                for half in (0, 1):
                    view = unit(plane_at(-d, 0) if half == 0 else plane_at(0, -d), half)
                    if not together:
                        arrived(view, first.at[half, j])
                    for e in AROUND:
                        send(kind, view, view, rest, there(half, 1, e))

        def end():
            arrived_rows(24 * rows, rest)

        return own, middle, end

    def x_unit(k):
        return lambda h, half: x_all.at[h, 64 * k + 32 * half : 64 * k + 32 * (half + 1)]

    def c_unit(h, half):
        return ct.at[h // 4, 4 * half : 4 * (half + 1), c, :, h % 4]

    def up_own():
        send(2, up_x, upb.at[seq], u_recv.at[8], partner)
        for i, j in ((1, 0), (7, 4)):
            send(2, upb.at[seq], upb.at[seq], u_recv.at[j], at(dz=i))
            send(2, up_x, upb.at[seq], u_recv.at[j], at(dz=i, core=other))

    def up_two():
        pl.semaphore_wait(alive.at[0], 2)
        for i in (2, 6):
            pl.semaphore_signal(alive.at[1], inc=1, device_id=at(dz=i), device_id_type=MESH)
        for i, j in ((2, 1), (6, 5)):
            send(2, upb.at[seq], upb.at[seq], u_recv.at[j], at(dz=i))
            send(2, up_x, upb.at[seq], u_recv.at[j], at(dz=i, core=other))

    def up_hop(d):
        below_, above_ = zs[8 - d] * 2, zs[d] * 2
        count = 2 if d < 4 else 1
        arrived(upb.at[0:count], u_recv.at[d - 1])
        if d in (2, 3):
            for parity in (c, other) if d < 3 else (c,):
                send(2, upb.at[below_ + parity], upb.at[below_ + parity], u_recv.at[d], at(dz=1))
        arrived(upb.at[0:count], u_recv.at[4 + d - 1])
        if d in (2, 3):
            for parity in (c, other) if d < 3 else (other,):
                send(2, upb.at[above_ + parity], upb.at[above_ + parity], u_recv.at[4 + d], at(dz=7))

    def g_send(src, s, k, down, d, p, core):
        send(3, src, qkv.at[s, k], g_recv.at[((down * 4 + d) * 2 + p) * 2 + k], at(dz=7 if down else 1, core=core))

    def g_own_first(k):
        g_send(qkv.at[seq, k], seq, k, 0, 0, 0, c)
        g_send(qkv_x.at[k], seq, k, 1, 0, 1, other)
        send(3, qkv_x.at[k], qkv.at[seq, k], g_mate.at[k], partner)

    def g_own_second(k):
        g_send(qkv_x.at[k], seq, k, 0, 0, 1, other)
        g_send(qkv.at[seq, k], seq, k, 1, 0, 0, c)

    def g_from_mate():
        for k in (0, 1):
            arrived(qkv.at[z * 2 + other, k], g_mate.at[k])
        arrived(upb.at[z * 2 + other], u_recv.at[8])

    def below(d, p):
        return zs[8 - d] * 2 + (c if p == 0 else other)

    def above(d, p):
        return zs[d] * 2 + (other if p == 0 else c)

    def g_hop(d, p, k):
        for down, s, q in ((0, below(d, p), p), (1, above(d, p), 1 - p)):
            arrived(qkv.at[s, k], g_recv.at[((down * 4 + d - 1) * 2 + q) * 2 + k])
            if d < 3 or (d == 3 and p == 0):
                g_send(qkv.at[s, k], s, k, down, d, q, c)

    def project(k):
        for i in range(3):
            acc = dot(x_all[0, 64 * k : 64 * (k + 1)], w_all[i, 0:256, :], 1, 0)
            for h in range(1, 16):
                acc = acc + dot(x_all[h, 64 * k : 64 * (k + 1)], w_all[i, 256 * h : 256 * (h + 1), :], 1, 0)
            acc = acc.astype(BF16)
            qkv[seq, k, i] = jnp.where(c == 0, acc[:, :128], acc[:, 128:])
            qkv_x[k, i] = jnp.where(c == 0, acc[:, 128:], acc[:, :128])

    quarter, group = head // 4, head % 4

    def slice_of(zt, k):
        rows = pl.ds(pl.multiple_of(64 * k + 16 * group, 16), 16)
        return x_all.at[2 * zt + quarter // 2, rows, lanes(quarter % 2)]

    own_slices = []

    def slices_out(k):
        own_slices.append(fetch(slice_of(z, k), ct.at[quarter, z, c, k, group], k))
        for i in (4, 3, 5, 2, 6, 1, 7):
            send(3, slice_of(zs[i], k), ct.at[quarter, z, c, k, group], z_recv.at[0], at(dz=i))

    a_own, a_mid, a_end = zip(*[plane(0, x_unit(k), 32, x_first.at[k], x_rest.at[k]) for k in (0, 1)])
    c_own, c_mid, c_end = plane(0, c_unit, 64, c_first, c_rest, together=True)

    a_own[0]()

    own_ldt.wait()
    total = jnp.concatenate([ldt[...], jnp.zeros((6, 128), F32)], axis=0)
    lane = lax.broadcasted_iota(jnp.int32, (8, 128), 1)
    for k in (1, 2, 4, 8, 16, 32, 64):
        total = total + jnp.where(lane >= k, pltpu.roll(total, k, 1), 0.0)

    def in_parts(row):
        hi = row.astype(BF16)
        rest = row - hi.astype(F32)
        mid = rest.astype(BF16)
        low = (rest - mid.astype(F32)).astype(BF16)
        return jnp.concatenate([hi.astype(F32), mid.astype(F32), low.astype(F32), jnp.zeros((5, 128), F32)], axis=0).astype(BF16)

    lo, hi = in_parts(total[0:1]), in_parts(total[1:2])
    upb[seq, 128:136] = jnp.where(c == 0, lo, hi)
    up_x[128:136] = jnp.where(c == 0, hi, lo)

    own_up.wait()
    oth_up.wait()
    a_own[1]()
    up_own()
    up_two()
    a_mid[0]()
    a_mid[1]()
    up_hop(1)
    pl.when(c == 0)(lambda: up_hop(2))
    pltpu.make_async_copy(w_all, w_all, loc.at[7]).wait()
    seg_v.wait()
    seg_s.wait()
    a_end[0]()
    pl.semaphore_wait(alive.at[1], 2)
    slices_out(0)
    project(0)
    g_own_first(0)
    pl.when(c == 1)(lambda: up_hop(2))
    a_end[1]()

    slices_out(1)
    project(1)
    g_own_first(1)
    g_own_second(0)
    g_own_second(1)
    g_from_mate()

    ti = lax.broadcasted_iota(jnp.int32, (128, 128), 0)
    si = lax.broadcasted_iota(jnp.int32, (128, 128), 1)

    def part(b, i):
        return jnp.concatenate([qkv[b, 0, i], qkv[b, 1, i]], axis=0)

    def prepared(b):
        parts = upb[b, 128:136].astype(F32)
        row = parts[0:1] + parts[1:2] + parts[2:3]
        before = segs[jnp.maximum(b * 128 - 1, 0)]
        previous = jnp.where(b > 0, before, -1).astype(F32)
        last = segs[b * 128 + 127].astype(F32)
        ls_s = jnp.broadcast_to(row, (128, 128))
        ls_t = ls_s.T
        seg_s = jnp.broadcast_to(segv[pl.ds(b, 1), :], (128, 128)).astype(F32)
        seg_t = seg_s.T
        same = (seg_s == seg_t) & (ti >= si)
        decay = jnp.where(same, SCALE * jnp.exp(jnp.where(same, ls_t - ls_s, 0.0)), 0.0)
        ls_last = row[:, 127:128]
        inflow = jnp.where(seg_t == previous, jnp.exp(ls_t), 0.0)
        outflow = jnp.where(seg_t == last, jnp.exp(ls_last - ls_t), 0.0)
        keep = jnp.where(last == previous, jnp.exp(ls_last), 0.0)
        return decay, inflow, outflow, jnp.broadcast_to(keep, (8, 128))

    def prepare(blocks):
        for j, b in enumerate(blocks):
            dec[j], inm[b], outm[b], carry[b] = prepared(b)

    def attend(blocks, ready=False):
        done = []
        for j, b in enumerate(blocks):
            q, k, v, u = part(b, 0), part(b, 1), part(b, 2), upb[b, 0:128]
            if ready:
                decay, inflow, outflow, keep = dec[j], inm[b], outm[b], None
            else:
                decay, inflow, outflow, keep = prepared(b)
            a_qk = (decay * dot(q, k, 1, 1)).astype(BF16)
            a_up = (decay * dot(u, v, 1, 1)).astype(BF16)
            wk_ = (SCALE * outflow * k.astype(F32)).astype(BF16)
            wq_ = (SCALE * inflow * q.astype(F32)).astype(BF16)
            done.append((
                inflow, outflow, keep, dot(a_up, k, 1, 0), dot(a_up, q, 0, 0),
                dot(a_qk, u, 0, 0), dot(wk_, v, 0, 0), dot(wq_, u, 0, 0),
            ))
        for b, (inflow, outflow, keep, gq, gk, gv, ls, rs) in zip(blocks, done):
            if not ready:
                inm[b], outm[b], carry[b] = inflow, outflow, keep
            gl[b, 0], gl[b, 1], gl[b, 2] = gq, gk, gv
            lst[b], rst[b] = ls, rs

    def c_begin():
        for copy in own_slices:
            copy.wait()
        arrived_rows(7 * 16, z_recv.at[0])
        c_own()

    def c_share():
        c_end()
        for i in (0, 1):
            view = ct.at[2 * i : 2 * i + 2, :, c]
            send(1, view, view, d_recv.at[i], partner)

    def block(j):
        return (z * 2 + 10 + j) % 16

    def scan(i, states):
        ahead, back = states
        b, e = block(i), block(29 - i)
        inc[b], ret[e] = ahead.astype(BF16), back.astype(BF16)
        return carry[b][0:1] * ahead + lst[b], carry[e][0:1] * back + rst[e]

    def finish(start, count):
        def run(i, carry_):
            done = []
            for b in [block(start + count * i + j) for j in range(count)]:
                inflow, outflow = inm[b], outm[b]
                done.append((b, (
                    gl[b, 0] + inflow * dot(upb[b, 0:128], inc[b], 1, 1),
                    gl[b, 1] + outflow * dot(part(b, 2), ret[b], 1, 1),
                    gl[b, 2] + outflow * dot(part(b, 1), ret[b], 1, 0),
                )))
            for b, parts in done:
                for k, value in enumerate(parts):
                    grads[b // 2, b % 2, :, 128 * k : 128 * (k + 1)] = value.astype(BF16)
            return carry_
        return run

    last = (zs[4] * 2, zs[4] * 2 + 1)
    attend((seq, z * 2 + other))
    up_hop(3)
    for d in (1, 2, 3):
        g_hop(d, 0, 0)
        g_hop(d, 0, 1)
        if d == 1:
            c_begin()
        if d == 2:
            c_mid()
        attend((below(d, 0), above(d, 0)))
        if d == 3:
            up_hop(4)
            prepare(last)
        g_hop(d, 1, 0)
        g_hop(d, 1, 1)
        if d == 3:
            c_share()
        attend((below(d, 1), above(d, 1)))
    zero = jnp.zeros((128, 128), F32)
    states = lax.fori_loop(0, 10, scan, (zero, zero), unroll=5)
    finish(4, 6)(0, 0)
    g_hop(4, 0, 0)
    g_hop(4, 0, 1)
    attend(last, ready=True)
    lax.fori_loop(10, 20, scan, states, unroll=5)
    finish(10, 10)(0, 0)
    def rows_of(core, j):
        return dot(ct[2 * core + j].reshape(2048, 128), grads[...].reshape(2048, 384), 0, 0).astype(BF16)

    for i in (0, 1):
        arrived(ct.at[2 * i : 2 * i + 2, :, other], d_recv.at[i])
    for j in (0, 1):
        rows_x[j] = rows_of(other, j)
        send(3, rows_x.at[j], rows_r.at[j], o_recv.at[j], partner)
    for j in (0, 1):
        mine = rows_of(c, j)
        for i in range(3):
            out[i, 128 * j : 128 * (j + 1), lanes(c)] = mine[:, 128 * i : 128 * (i + 1)]
    for j in (0, 1):
        arrived(rows_r.at[j], o_recv.at[j])
        for i in range(3):
            out[i, 128 * j : 128 * (j + 1), lanes(other)] = rows_r[j, :, 128 * i : 128 * (i + 1)]
    for kind, rows in sent.items():
        view = upb.at[0:15] if kind == 2 else w_all.at[0, 0:rows]
        pltpu.make_async_remote_copy(
            src_ref=view, dst_ref=view, send_sem=sends.at[kind], recv_sem=loc.at[0], device_id=partner, device_id_type=MESH
        ).wait_send()


def local(tokens, w_query, w_key, w_value, upstream, log_decay, segment):
    hbm = pl.BlockSpec(memory_space=pltpu.HBM)
    dma = pltpu.SemaphoreType.DMA
    out = pl.pallas_call(
        kernel,
        out_shape=jax.ShapeDtypeStruct((3, 256, 256), BF16),
        in_specs=[hbm] * 8,
        out_specs=pl.BlockSpec(memory_space=pltpu.VMEM),
        scratch_shapes=[
            pltpu.VMEM((2, 128), F32),
            pltpu.VMEM((16, 128), jnp.int32),
            pltpu.SMEM((2048,), jnp.int32),
            pltpu.VMEM((16, 128, 256), BF16),
            pltpu.VMEM((3, 4096, 256), BF16),
            pltpu.VMEM((16, 2, 3, 64, 128), BF16),
            pltpu.VMEM((2, 3, 64, 128), BF16),
            pltpu.VMEM((16, 136, 128), BF16),
            pltpu.VMEM((136, 128), BF16),
            pltpu.VMEM((4, 8, 2, 2, 4, 16, 128), BF16),
            pltpu.VMEM((16, 3, 128, 128), F32),
            pltpu.VMEM((16, 128, 128), F32),
            pltpu.VMEM((16, 128, 128), F32),
            pltpu.VMEM((16, 8, 128), F32),
            pltpu.VMEM((2, 128, 128), F32),
            pltpu.VMEM((16, 128, 128), F32),
            pltpu.VMEM((16, 128, 128), F32),
            pltpu.VMEM((16, 128, 128), BF16),
            pltpu.VMEM((16, 128, 128), BF16),
            pltpu.VMEM((8, 2, 128, 384), BF16),
            pltpu.VMEM((2, 128, 384), BF16),
            pltpu.VMEM((2, 128, 384), BF16),
            dma((2, 2, 3)), dma((2,)),
            dma((1,)), dma(()),
            dma((1,)), dma((9,)),
            dma((2,)), dma((32,)),
            dma((2,)), dma((2,)),
            dma((4,)), dma((8,)),
            pltpu.SemaphoreType.REGULAR((2,)),
        ],
        compiler_params=pltpu.CompilerParams(
            collective_id=0, has_side_effects=True, vmem_limit_bytes=40 * 1024 * 1024
        ),
    )(*[
        pltpu.with_memory_space_constraint(a, pltpu.HBM)
        for a in (
            tokens, w_query, w_key, w_value, upstream,
            log_decay.T, segment.reshape(16, 128), segment,
        )
    ])
    return out[0], out[1], out[2]


def solution(mesh):
    in_specs = (
        P("seq", "head"), P(None, "head"), P(None, "head"), P(None, "head"),
        P("seq", "head"), P("seq", "head"), P(),
    )
    out_specs = (P("seq", "head"),) * 3
    return jax.shard_map(local, mesh=mesh, in_specs=in_specs, out_specs=out_specs, check_vma=False)
```
